32 devices in a mesh: dp: 8 (over y, x, core), tp: 4 (over z).
Axes of the slice: x: 2, y: 2, z: 4, core: 2. Of those that a mesh axis runs over, the one named last changes fastest.
Arguments:
- tokens: bfloat16 [128, 8192], P('tp', 'dp'), may hold values from -6 to 6
- targets: bfloat16 [128, 8192], P('tp', 'dp'), may hold values from -6 to 6
- gate_weight: bfloat16 [8192, 16384], P('dp', 'tp'), may hold values from -0.0625 to 0.0625
- up_weight: bfloat16 [8192, 16384], P('dp', 'tp'), may hold values from -0.0625 to 0.0625
- down_weight: bfloat16 [16384, 8192], P('tp', 'dp'), may hold values from -0.046875 to 0.046875
- direction_gate: bfloat16 [8192, 16384], P('dp', 'tp'), may hold values from -36 to 36
- direction_up: bfloat16 [8192, 16384], P('dp', 'tp'), may hold values from -36 to 36
- direction_down: bfloat16 [16384, 8192], P('tp', 'dp'), may hold values from -36 to 36
- previous_gate: bfloat16 [8192, 16384], P('dp', 'tp'), may hold values from -36 to 36
- previous_up: bfloat16 [8192, 16384], P('dp', 'tp'), may hold values from -36 to 36
- previous_down: bfloat16 [16384, 8192], P('tp', 'dp'), may hold values from -36 to 36
- beta_prev: float32 [1], replicated, may hold values from 1 to 4
Outputs:
- next_gate: bfloat16 [8192, 16384], P('dp', 'tp')
- next_up: bfloat16 [8192, 16384], P('dp', 'tp')
- next_down: bfloat16 [16384, 8192], P('tp', 'dp')
- coefficients: float32 [2], replicated
The draws below stay inside these ranges and needn't reach their ends.
All inputs are finite; a program needn't handle non-finite values.
Results may differ from the reference program's by a relative error of at most 0.015.
Values may be sent and summed in bfloat16 or wider, within the bound.
A program may use at most 256 MiB of HBM per device.

```python
import math
import jax
import jax.numpy as jnp
from jax import lax

D = 8192
FF = 16384
TOKENS = 128


def rising_field(key, salt, rows, cols, width_dim):
    sub = jax.random.fold_in(key, salt)
    base = jnp.clip(jax.random.normal(sub, (rows, cols), jnp.float32), -6.0, 6.0)
    ratio = 6.0
    count = rows if width_dim == 0 else cols
    place = jnp.arange(count, dtype=jnp.float32) / max(count - 1, 1)
    factor = jnp.exp(place * math.log(ratio))
    if width_dim == 0:
        return (base * factor[:, None]).astype(jnp.bfloat16)
    return (base * factor[None, :]).astype(jnp.bfloat16)


def draw_direction_gate(key, part):
    return rising_field(key, 11, D, FF, 0)


def draw_direction_up(key, part):
    return rising_field(key, 12, D, FF, 0)


def draw_direction_down(key, part):
    return rising_field(key, 13, FF, D, 1)


def draw_previous_gate(key, part):
    return rising_field(key, 21, D, FF, 0)


def draw_previous_up(key, part):
    return rising_field(key, 22, D, FF, 0)


def draw_previous_down(key, part):
    return rising_field(key, 23, FF, D, 1)


def level_of(rng, dims, split, low, high):
    def one(position, blocks):
        steps = jax.random.uniform(jax.random.fold_in(jax.random.fold_in(rng, 6), position), (blocks,), jnp.float32, low / len(split), high / len(split))
        return jnp.repeat(jnp.exp(steps), dims[position] // blocks).reshape((-1,) + (1,) * (len(dims) - position - 1))

    loudness = one(*split[0])
    for cut in split[1:]:
        loudness = loudness * one(*cut)
    return loudness


def gaussian(own_key, dims, spread, most, split=(), kind=jnp.bfloat16):
    gain = level_of(own_key, dims, split, -0.22, 0.18) if split else 1.0
    values = jax.random.normal(own_key, dims, jnp.float32) * spread * gain
    return jnp.minimum(jnp.maximum(values, -most), most).astype(kind)


def setup_inputs(seed: int = 0) -> dict:
    arg_keys = jax.random.split(jax.random.key(seed), 13)
    return {
        "tokens": gaussian(arg_keys[0], (TOKENS, D), 1.0, 6.0, ((0, 4), (1, 8))),
        "targets": gaussian(arg_keys[1], (TOKENS, D), 1.0, 6.0, ((0, 4), (1, 8))),
        "gate_weight": gaussian(arg_keys[2], (D, FF), D ** -0.5, 0.0625, ((0, 8), (1, 4))),
        "up_weight": gaussian(arg_keys[3], (D, FF), D ** -0.5, 0.0625, ((0, 8), (1, 4))),
        "down_weight": gaussian(arg_keys[4], (FF, D), FF ** -0.5, 0.046875, ((0, 4), (1, 8))),
        "direction_gate": draw_direction_gate(jax.random.fold_in(arg_keys[12], 71), 0),
        "direction_up": draw_direction_up(jax.random.fold_in(arg_keys[12], 71), 0),
        "direction_down": draw_direction_down(jax.random.fold_in(arg_keys[12], 71), 0),
        "previous_gate": draw_previous_gate(jax.random.fold_in(arg_keys[12], 71), 0),
        "previous_up": draw_previous_up(jax.random.fold_in(arg_keys[12], 71), 0),
        "previous_down": draw_previous_down(jax.random.fold_in(arg_keys[12], 71), 0),
        "beta_prev": jnp.clip(jax.random.uniform(arg_keys[11], (1,), jnp.float32, 1.0, 4.0), 1.0, 4.0),
    }


def product(first_op, second_op):
    return jnp.dot(first_op, second_op, preferred_element_type=jnp.float32)

def against(first_op, second_op):
    return lax.dot_general(first_op, second_op, (((1,), (1,)), ((), ())), preferred_element_type=jnp.float32)

def transposed(first_op, second_op):
    return lax.dot_general(first_op, second_op, (((0,), (0,)), ((), ())), preferred_element_type=jnp.float32)

def pointwise(gate_sum):
    logistic = jax.nn.sigmoid(gate_sum)
    activation = gate_sum * logistic
    gate_slope = logistic * (1.0 + gate_sum * (1.0 - logistic))
    gate_curve = logistic * (1.0 - logistic) * (2.0 + gate_sum * (1.0 - 2.0 * logistic))
    return (activation, gate_slope, gate_curve)

def reference(tokens, targets, gate_weight, up_weight, down_weight, direction_gate, direction_up, direction_down, previous_gate, previous_up, previous_down, beta_prev):
    gate_sum = product(tokens, gate_weight)
    up_sum = product(tokens, up_weight)
    gate_dir = product(tokens, direction_gate)
    up_dir = product(tokens, direction_up)
    activation, gate_slope, gate_curve = pointwise(gate_sum)
    hidden = (activation * up_sum).astype(jnp.bfloat16)
    hidden_dir = (gate_slope * up_sum * gate_dir + activation * up_dir).astype(jnp.bfloat16)
    output = product(hidden, down_weight)
    output_dir = product(hidden_dir, down_weight) + product(hidden, direction_down)
    total_rows = tokens.shape[0]
    grad_out = ((output - targets.astype(jnp.float32)) / total_rows).astype(jnp.bfloat16)
    grad_out_dir = (output_dir / total_rows).astype(jnp.bfloat16)
    grad_hidden = against(grad_out, down_weight)
    grad_hidden_dir = against(grad_out_dir, down_weight) + against(grad_out, direction_down)
    grad_gate_dir = (grad_hidden_dir * up_sum * gate_slope + grad_hidden * up_dir * gate_slope + grad_hidden * up_sum * gate_curve * gate_dir).astype(jnp.bfloat16)
    grad_up_dir = (grad_hidden_dir * activation + grad_hidden * gate_slope * gate_dir).astype(jnp.bfloat16)
    image_gate = transposed(tokens, grad_gate_dir)
    image_up = transposed(tokens, grad_up_dir)
    image_down = transposed(hidden_dir, grad_out) + transposed(hidden, grad_out_dir)
    images = [image_gate, image_up, image_down]
    alongs = [matrix.astype(jnp.float32) for matrix in (direction_gate, direction_up, direction_down)]
    befores = [matrix.astype(jnp.float32) for matrix in (previous_gate, previous_up, previous_down)]
    entries = 3 * D * FF
    alpha_coef = sum((jnp.sum(image_part * along_part) for image_part, along_part in zip(images, alongs))) / entries
    beta_old = beta_prev[0]
    residuals = [image_part - alpha_coef * along_part - beta_old * before_part for image_part, along_part, before_part in zip(images, alongs, befores)]
    beta_coef = jnp.sqrt(sum((jnp.sum(matrix * matrix) for matrix in residuals)) / entries + 1e-06)
    next_parts = [(matrix / beta_coef).astype(jnp.bfloat16) for matrix in residuals]
    return (next_parts[0], next_parts[1], next_parts[2], jnp.stack([alpha_coef, beta_coef]).astype(jnp.float32))
```

```python
import functools

import jax
import jax.numpy as jnp
from jax import lax
from jax.experimental import pallas as pl
from jax.experimental.pallas import tpu as pltpu
from jax.sharding import PartitionSpec as P

MESH = pl.DeviceIdType.MESH
VMEM = pltpu.VMEM
DMA = pltpu.SemaphoreType.DMA
ANY = pl.BlockSpec(memory_space=pl.ANY)
WHOLE = pl.BlockSpec(memory_space=pltpu.VMEM)
F32 = jnp.float32
BF16 = jnp.bfloat16
LIMIT = 62 * 1024 * 1024


def tile_of(size, most):
    tile = min(size, most)
    while size % tile:
        tile //= 2
    return tile


def dot(one, two):
    return jnp.dot(one, two, preferred_element_type=F32)


def against(one, two):
    return lax.dot_general(one, two, (((1,), (1,)), ((), ())), preferred_element_type=F32)


def greet(targets):
    barrier = pltpu.get_barrier_semaphore()
    for target in targets:
        pl.semaphore_signal(barrier, inc=1, device_id=target, device_id_type=MESH)
    pl.semaphore_wait(barrier, len(targets))


def remote(src, dst, send_sem, recv_sem, target):
    return pltpu.make_async_remote_copy(
        src_ref=src, dst_ref=dst, send_sem=send_sem, recv_sem=recv_sem, device_id=target, device_id_type=MESH
    )


def folded(values, width=None):
    rows, cols = values.shape
    return values.reshape(rows // 8, 8, cols).sum(axis=0)


def lanes(values):
    total = values[:, :128]
    for at in range(128, values.shape[1], 128):
        total = total + values[:, at : at + 128]
    return total


class Width:
    def __init__(self, n, phases, chunks, kinds, share, width):
        self.n, self.phases, self.chunks, self.kinds = n, phases, chunks, kinds
        self.share, self.width = share, width
        self.steps = phases * chunks
        self.ys, self.xs = 2, n // 4
        self.step = width // chunks

    def scratch(self):
        p, y, x, share, width, v = self.phases, self.ys, self.xs, self.share, self.width, self.steps
        return [
            VMEM((p, 2, y, x, 2, share, width), BF16),
            VMEM((p, 2, y, x, share, width), BF16),
            VMEM((p, 2, y, x, share, width), BF16),
            VMEM((p, x, y, share, width), BF16),
            VMEM((p, x, share, width), BF16),
            VMEM((p, share, width), BF16),
            VMEM((p, x, share, width), BF16),
            VMEM((p, share, width), BF16),
            VMEM((p, x, share, width), BF16),
            VMEM((self.kinds, y, x, 2, share, width), BF16),
        ] + [
            DMA((v,)), DMA((v,)),
            DMA((v, x)), DMA((v, x)),
            DMA((v,)), DMA((v,)),
            DMA((v,)), DMA((v,)),
            DMA((v, x)), DMA((v, x)),
            DMA((v, x)), DMA((v, x)),
            DMA((v,)), DMA((v,)),
            DMA((v, x)), DMA((v, x)),
            DMA((v, x)), DMA((v, x)),
            DMA((v, y * x)), DMA((v, y * x)),
        ]

    def bind(self, refs):
        (self.x, self.mate_in, self.paired, self.x1, self.y1, self.y2, self.x2, self.sa, self.sb, self.full) = refs[:10]
        sems = refs[10:]
        self.sems = [(sems[i], sems[i + 1]) for i in range(0, len(sems), 2)]
        me = lax.axis_index("dp")
        self.core = lax.rem(me, 2)
        chip = lax.div(me, 2)
        self.px, self.py = lax.rem(chip, self.xs), lax.div(chip, self.xs)
        self.qy = 1 - self.py
        self.mate = self.at(self.py, self.px, 1 - self.core)
        self.across = self.at(self.qy, self.px, self.core)
        self.to = [lax.rem(self.px + s, self.xs) for s in range(self.xs)]
        self.off = [lax.rem(self.px + self.xs - s, self.xs) for s in range(self.xs)]

    def at(self, y, x, core):
        return {"dp": (y * self.xs + x) * 2 + core}

    def partners(self):
        row = [self.at(self.py, self.to[s], self.core) for s in range(1, self.xs)]
        return [self.mate, self.across] + row

    def cols(self, v, part=0, parts=1):
        size = self.step // parts
        start = lax.rem(v, self.chunks) * self.step + part * size
        return pl.ds(pl.multiple_of(start, size), size)

    def phase(self, v):
        return lax.div(v, self.chunks)

    def row(self, s):
        return self.at(self.py, self.to[s], self.core)

    def mated(self, v):
        p, cols, (s, r) = self.phase(v), self.cols(v), self.sems[0]
        return remote(
            self.x.at[p, :, :, :, 1 - self.core, :, cols], self.mate_in.at[p, :, :, :, :, cols], s.at[v], r.at[v], self.mate
        )

    def first_x(self, v, k):
        p, cols, (s, r) = self.phase(v), self.cols(v), self.sems[1]
        return remote(
            self.paired.at[p, 0, :, self.to[k], :, cols], self.x1.at[p, self.px, :, :, cols], s.at[v, k], r.at[v, k], self.row(k)
        )

    def first_y(self, v):
        p, cols, (s, r) = self.phase(v), self.cols(v), self.sems[2]
        return remote(
            self.paired.at[p, 1, self.qy, :, :, cols], self.y1.at[p, :, :, cols], s.at[v], r.at[v], self.across
        )

    def second_y(self, v):
        p, cols, (s, r) = self.phase(v), self.cols(v), self.sems[3]
        return remote(self.sa.at[p, :, cols], self.y2.at[p, :, cols], s.at[v], r.at[v], self.across)

    def second_x(self, v, k):
        p, cols, (s, r) = self.phase(v), self.cols(v), self.sems[4]
        return remote(
            self.sb.at[p, self.to[k], :, cols], self.x2.at[p, self.px, :, cols], s.at[v, k], r.at[v, k], self.row(k)
        )

    def block(self, v, y, x):
        if self.phases > 1:
            return self.full.at[self.phase(v), y, x, self.core, :, self.cols(v)]
        return self.full.at[:, y, x, self.core, :, self.cols(v)]

    def half(self, v, y, x, part):
        if self.phases > 1:
            parts = 2 if self.step % 256 == 0 else 1
            if parts == 1:
                rows = pl.ds(part * (self.share // 2), self.share // 2)
                return self.full.at[self.phase(v), y, x, self.core, rows, self.cols(v)]
            return self.full.at[self.phase(v), y, x, self.core, :, self.cols(v, part, 2)]
        return self.full.at[part, y, x, self.core, :, self.cols(v)]

    def gather_x(self, v, k):
        s, r = self.sems[5]
        mine = self.block(v, self.py, self.px)
        return remote(mine, mine, s.at[v, k], r.at[v, k], self.row(k))

    def gather_y(self, v):
        s, r = self.sems[6]
        mine = self.block(v, self.py, self.px)
        return remote(mine, mine, s.at[v], r.at[v], self.across)

    def pass_y(self, v, k):
        s, r = self.sems[7]
        piece = self.half(v, self.py, self.off[k], 0)
        return remote(piece, piece, s.at[v, k], r.at[v, k], self.across)

    def pass_x(self, v, k):
        s, r = self.sems[8]
        piece = self.half(v, self.qy, self.px, 1)
        return remote(piece, piece, s.at[v, k], r.at[v, k], self.row(k))

    def hand(self, v, role):
        s, r = self.sems[9]
        y, k = (self.py, role) if role < self.xs else (self.qy, role - self.xs)
        piece = self.block(v, y, self.off[k])
        return remote(piece, piece, s.at[v, role], r.at[v, role], self.mate)

    def put(self, v, kind, rows):
        p, cols = self.phase(v), self.cols(v)
        shape = (self.ys, self.xs, 2, self.share, self.step)
        self.x[p, kind, :, :, :, :, cols] = rows.astype(BF16).reshape(shape)

    def pair(self, v):
        p, cols = self.phase(v), self.cols(v)
        self.mated(v).wait_recv()
        self.paired[p, :, :, :, :, cols] = (
            self.x[p, :, :, :, self.core, :, cols].astype(F32) + self.mate_in[p, :, :, :, :, cols].astype(F32)
        ).astype(BF16)
        for k in range(1, self.xs):
            self.first_x(v, k).start()
        self.first_y(v).start()

    def cross(self, v):
        p, cols = self.phase(v), self.cols(v)
        for k in range(1, self.xs):
            self.first_x(v, k).wait_recv()
        total = self.paired[p, 0, self.qy, self.px, :, cols].astype(F32)
        for k in range(1, self.xs):
            total = total + self.x1[p, self.off[k], self.qy, :, cols].astype(F32)
        self.sa[p, :, cols] = total.astype(BF16)
        self.second_y(v).start()
        self.first_y(v).wait_recv()
        for k in range(1, self.xs):
            total = self.paired[p, 1, self.py, self.to[k], :, cols].astype(F32) + self.y1[
                p, self.to[k], :, cols
            ].astype(F32)
            self.sb[p, self.to[k], :, cols] = total.astype(BF16)
            self.second_x(v, k).start()

    def totals(self, v):
        p, cols = self.phase(v), self.cols(v)
        self.second_y(v).wait_recv()
        for k in range(1, self.xs):
            self.second_x(v, k).wait_recv()
        one = self.paired[p, 0, self.py, self.px, :, cols].astype(F32) + self.y2[p, :, cols].astype(F32)
        two = self.paired[p, 1, self.py, self.px, :, cols].astype(F32) + self.y1[p, self.px, :, cols].astype(F32)
        for k in range(1, self.xs):
            one = one + self.x1[p, self.off[k], self.py, :, cols].astype(F32)
            two = two + self.x2[p, self.off[k], :, cols].astype(F32)
        return one, two

    def keep(self, v, kind, rows):
        self.full[kind, self.py, self.px, self.core, :, self.cols(v)] = rows.astype(BF16)

    def spread(self, v):
        for k in range(1, self.xs):
            self.gather_x(v, k).start()
        self.gather_y(v).start()
        self.hand(v, 0).start()

    def relay(self, v):
        for k in range(1, self.xs):
            self.gather_x(v, k).wait_recv()
            self.pass_y(v, k).start()
        self.gather_y(v).wait_recv()
        for k in range(1, self.xs):
            self.pass_x(v, k).start()
        for role in range(1, self.xs + 1):
            self.hand(v, role).start()

    def relay_last(self, v):
        for k in range(1, self.xs):
            self.pass_y(v, k).wait_recv()
            self.pass_x(v, k).wait_recv()
            self.hand(v, self.xs + k).start()

    def complete(self, v):
        for role in range(2 * self.xs):
            self.hand(v, role).wait_recv()

    def rows(self, v, kind):
        cols = self.cols(v)
        return self.full[kind, :, :, :, :, cols].reshape(self.n * self.share, self.step)

    def drain(self):
        @pl.loop(0, self.steps)
        def _(v):
            self.mated(v).wait_send()
            self.first_y(v).wait_send()
            self.second_y(v).wait_send()
            self.gather_y(v).wait_send()
            for k in range(1, self.xs):
                for copy in (self.first_x, self.second_x, self.gather_x, self.pass_y, self.pass_x):
                    copy(v, k).wait_send()
            for role in range(2 * self.xs):
                self.hand(v, role).wait_send()


LAGS = dict(pair=1, cross=3, totals=5, relay=7, last=9, done=10)


def staged(i, lag, steps, body):
    v = i - lag

    @pl.when((v >= 0) & (v < steps))
    def _():
        body(v)


DEEP = 4
SLOTS = 3


def squares(along_ref, before_ref, norms):
    rows, width = along_ref.shape
    step = tile_of(rows, 32)

    def body(i, sums):
        at = pl.ds(pl.multiple_of(i * step, step), step)
        along = along_ref[at, :].astype(F32)
        before = before_ref[at, :].astype(F32)
        products = (along * along, along * before, before * before)
        return tuple(have + folded(product) for have, product in zip(sums, products))

    zero = jnp.zeros((8, width), F32)
    sums = lax.fori_loop(0, rows // step, body, (zero, zero, zero))
    for kind in range(3):
        norms[kind] += lanes(sums[kind])


def early_kernel(n, t, width, *refs):
    (tokens, targets, gate, up, down, along_gate, along_up, along_down, before_gate, before_up, before_down) = refs[:11]
    (out_tokens, out_units, out_keeps, out_grads, out_before, norms) = refs[11:17]
    (tok, keeps, bx, weights, downs, alongs, wide, tall, acc, zx, zin, gz) = refs[17:29]
    (tok_s, tok_r, w_sem, d_sem, wide_sem, tall_sem, zs, zr, gs, gr, o_sem) = refs[29:40]
    width.bind(refs[40:])
    chunks, steps, step = width.chunks, width.steps, width.step
    share, depth = tokens.shape
    rows = t * share
    me = lax.axis_index("tp")
    spots = [lax.rem(me + s, t) for s in range(1, t)]
    sources = [lax.rem(me + t - s, t) for s in range(1, t)]

    def col(v):
        return width.cols(v)

    def load(v, one, two, start):
        slot = lax.rem(v, DEEP)
        for kind, ref in enumerate((one, two)):
            copy = pltpu.make_async_copy(ref.at[:, col(v)], weights.at[slot, kind], w_sem.at[slot, kind])
            if start:
                copy.start()
            else:
                copy.wait()

    def fetch(v):
        @pl.when(v < chunks)
        def _():
            load(v, gate, up, True)

        @pl.when((v >= chunks) & (v < steps))
        def _():
            load(v, along_gate, along_up, True)

    for v in range(DEEP):
        fetch(jnp.int32(v))

    def wide_copies(one, two, c):
        slot = lax.rem(c, SLOTS)
        return [
            pltpu.make_async_copy(ref.at[:, col(c)], wide.at[slot, kind], wide_sem.at[slot, kind])
            for kind, ref in enumerate((one, two))
            if ref is not None
        ]

    def tall_copies(c):
        slot = lax.rem(c, SLOTS)
        return [
            pltpu.make_async_copy(ref.at[col(c), :], tall.at[slot, kind], tall_sem.at[slot, kind])
            for kind, ref in enumerate((along_down, before_down))
        ]

    def open_stream(copies):
        for c in range(min(SLOTS, chunks)):
            for copy in copies(jnp.int32(c)):
                copy.start()

    def run_stream(copies, body):
        @pl.loop(0, chunks)
        def _(c):
            for copy in copies(c):
                copy.wait()
            body(c, lax.rem(c, SLOTS))

            @pl.when(c + SLOTS < chunks)
            def _():
                for copy in copies(c + SLOTS):
                    copy.start()

    gate_stream = functools.partial(wide_copies, along_gate, before_gate)
    up_stream = functools.partial(wide_copies, along_up, before_up)
    again_stream = functools.partial(wide_copies, None, before_gate)
    open_stream(gate_stream)
    load_down = pltpu.make_async_copy(down, downs, d_sem.at[0])
    load_along = pltpu.make_async_copy(along_down, alongs, d_sem.at[1])

    norms[...] = jnp.zeros_like(norms)
    greet(width.partners() + [{"tp": spot} for spot in spots])

    def gather(i):
        return remote(tokens, tok.at[me], tok_s.at[i], tok_r.at[i], {"tp": spots[i]})

    for i in range(t - 1):
        gather(i).start()
    tok[me] = tokens[...]

    def norm_wide(c, slot):
        squares(wide.at[slot, 0], wide.at[slot, 1], norms)

    run_stream(gate_stream, norm_wide)
    load_down.start()
    load_along.start()
    for i in range(t - 1):
        gather(i).wait_recv()

    def everyone():
        return tok[...].reshape(rows, depth)

    acc[...] = jnp.zeros_like(acc)

    def front(v):
        load(v, gate, up, False)
        slot = lax.rem(v, DEEP)
        for kind in range(2):
            width.put(v, kind, dot(everyone(), weights[slot, kind]))
        width.mated(v).start()
        fetch(v + DEEP)

    def sums(v):
        one, two = width.totals(v)
        cols = col(v)
        p = width.phase(v)

        @pl.when(p == 0)
        def _():
            keeps[0, :, cols] = one
            keeps[1, :, cols] = two
            width.keep(v, 0, one * jax.nn.sigmoid(one) * two)

        @pl.when(p == 1)
        def _():
            keeps[2, :, cols] = one
            keeps[3, :, cols] = two
            gate_sum, up_sum = keeps[0, :, cols], keeps[1, :, cols]
            logistic = jax.nn.sigmoid(gate_sum)
            slope = logistic * (1.0 + gate_sum * (1.0 - logistic))
            width.keep(v, 1, slope * up_sum * one + gate_sum * logistic * two)

        width.spread(v)

    def middle(v):
        width.complete(v)
        p, at = width.phase(v), col(v)

        @pl.when(v == 0)
        def _():
            load_down.wait()

        @pl.when(v == chunks)
        def _():
            load_along.wait()

        @pl.when(p == 0)
        def _():
            acc[0] += dot(width.rows(v, 0), downs[at, :])

        @pl.when(p == 1)
        def _():
            acc[1] += dot(width.rows(v, 1), downs[at, :]) + dot(width.rows(v, 0), alongs[at, :])

    def z_first(p, i):
        return remote(zx.at[p, spots[i]], zin.at[p, me], zs.at[p, i], zr.at[p, i], {"tp": spots[i]})

    def z_second(p, i):
        return remote(gz.at[p, me], gz.at[p, me], gs.at[p, i], gr.at[p, i], {"tp": spots[i]})

    def z_send(p):
        zx[p] = acc[p].astype(BF16).reshape(t, share, depth)
        for i in range(t - 1):
            z_first(p, i).start()

    def z_finish(p):
        for i in range(t - 1):
            z_first(p, i).wait_recv()
        total = zx[p, me].astype(F32)
        for at in sources:
            total = total + zin[p, at].astype(F32)
        if p == 0:
            total = total - targets[...].astype(F32)
        gz[p, me] = (total / rows).astype(BF16)
        for i in range(t - 1):
            z_second(p, i).start()

    ready = chunks - 1 + LAGS["done"]
    last = steps + LAGS["done"]
    settle = min(ready + 6, last - 1)

    @pl.loop(0, last)
    def _(i):
        staged(i, 0, steps, front)
        staged(i, LAGS["cross"], steps, width.cross)
        staged(i, LAGS["totals"], steps, sums)
        staged(i, LAGS["relay"], steps, width.relay)
        staged(i, LAGS["last"], steps, width.relay_last)
        staged(i, LAGS["done"], steps, middle)
        staged(i, LAGS["pair"], steps, width.pair)

        @pl.when(i == ready)
        def _():
            z_send(0)

        @pl.when(i == settle)
        def _():
            z_finish(0)

    z_send(1)
    open_stream(up_stream)

    def before_of(kind):
        def body(c, slot):
            bx[kind, :, col(c)] = dot(everyone(), wide[slot, 1]).astype(BF16)

        return body

    def norm_and_before(c, slot):
        norm_wide(c, slot)
        before_of(1)(c, slot)

    stores = [
        pltpu.make_async_copy(tok, out_tokens, o_sem.at[0]),
        pltpu.make_async_copy(width.full, out_units, o_sem.at[1]),
        pltpu.make_async_copy(keeps, out_keeps, o_sem.at[2]),
    ]
    for store in stores:
        store.start()
    run_stream(up_stream, norm_and_before)
    open_stream(tall_copies)
    open_stream(again_stream)
    z_finish(1)

    def norm_tall(c, slot):
        squares(tall.at[slot, 0], tall.at[slot, 1], norms)

    run_stream(tall_copies, norm_tall)
    run_stream(again_stream, before_of(0))
    stores.append(pltpu.make_async_copy(bx, out_before, o_sem.at[3]))
    stores[-1].start()
    for p in range(2):
        for i in range(t - 1):
            z_second(p, i).wait_recv()
    stores.append(pltpu.make_async_copy(gz, out_grads, o_sem.at[4]))
    stores[-1].start()
    for i in range(t - 1):
        gather(i).wait_send()
        for p in range(2):
            z_first(p, i).wait_send()
            z_second(p, i).wait_send()
    width.drain()
    for store in stores:
        store.wait()


def early(n, t, tokens, targets, gate, up, down, along_gate, along_up, along_down, before_gate, before_up, before_down):
    share, depth = tokens.shape
    width = gate.shape[1]
    rows = t * share
    chunks = width // tile_of(width, max(128, width // 8))
    plan = Width(n, 2, chunks, 2, rows // n, width)
    step = plan.step
    keeps = (4, plan.share, width)
    units = (2, plan.ys, plan.xs, 2, plan.share, width)
    z = (2, t, share, depth)
    return pl.pallas_call(
        functools.partial(early_kernel, n, t, plan),
        out_shape=[
            jax.ShapeDtypeStruct((t, share, depth), BF16),
            jax.ShapeDtypeStruct(units, BF16),
            jax.ShapeDtypeStruct(keeps, F32),
            jax.ShapeDtypeStruct(z, BF16),
            jax.ShapeDtypeStruct((2, rows, width), BF16),
            jax.ShapeDtypeStruct((3, 8, 128), F32),
        ],
        in_specs=[WHOLE, WHOLE] + [ANY] * 9,
        out_specs=[ANY] * 5 + [WHOLE],
        scratch_shapes=[
            VMEM((t, share, depth), BF16),
            VMEM(keeps, F32),
            VMEM((2, rows, width), BF16),
            VMEM((DEEP, 2, depth, step), BF16),
            VMEM((width, depth), BF16),
            VMEM((width, depth), BF16),
            VMEM((SLOTS, 2, depth, step), BF16),
            VMEM((SLOTS, 2, step, depth), BF16),
            VMEM((2, rows, depth), F32),
            VMEM(z, BF16),
            VMEM(z, BF16),
            VMEM(z, BF16),
            DMA((t - 1,)),
            DMA((t - 1,)),
            DMA((DEEP, 2)),
            DMA((2,)),
            DMA((SLOTS, 2)),
            DMA((SLOTS, 2)),
            DMA((2, t - 1)),
            DMA((2, t - 1)),
            DMA((2, t - 1)),
            DMA((2, t - 1)),
            DMA((5,)),
        ]
        + plan.scratch(),
        compiler_params=pltpu.CompilerParams(collective_id=1, has_side_effects=True, vmem_limit_bytes=LIMIT),
    )(tokens, targets, gate, up, down, along_gate, along_up, along_down, before_gate, before_up, before_down)


def late_kernel(n, t, entries, width, *refs):
    (tokens, units, keeps_in, grads_in, before_in, norms, down, along, before, beta_prev) = refs[:10]
    (out_dirs, scales) = refs[10:12]
    (grads, hidden, keeps, bx, downs, alongs, befores, sums, gram, swap_gram) = refs[12:22]
    (dp_in, total_dp, tp_in) = refs[22:25]
    (in_sem, m_sem, o_sem, s1, r1, s2, r2) = refs[25:32]
    width.bind(refs[32:])
    chunks, steps, step = width.chunks, width.steps, width.step
    depth = down.shape[1]
    rows = n * width.share
    dp, tp = lax.axis_index("dp"), lax.axis_index("tp")
    dp_spots = [lax.rem(dp + s, n) for s in range(1, n)]
    tp_spots = [lax.rem(tp + s, t) for s in range(1, t)]

    loads = [
        pltpu.make_async_copy(src, dst, in_sem.at[i])
        for i, (src, dst) in enumerate(((grads_in, grads), (units, hidden), (keeps_in, keeps), (before_in, bx)))
    ]

    def matrix(which, c):
        src, dst = ((down, downs), (along, alongs), (before, befores))[which]
        at = width.cols(c)
        return pltpu.make_async_copy(src.at[at, :], dst.at[at, :], m_sem.at[which, c])

    loads[0].start()
    for c in range(chunks):
        matrix(0, jnp.int32(c)).start()
        matrix(1, jnp.int32(c)).start()
        if c == 0:
            for load in loads[1:]:
                load.start()
    for c in range(chunks):
        matrix(2, jnp.int32(c)).start()
    sums[...] = jnp.zeros_like(sums)
    gram[...] = jnp.zeros_like(gram)
    swap_gram[...] = jnp.zeros_like(swap_gram)
    greet([{"dp": spot} for spot in dp_spots] + [{"tp": spot} for spot in tp_spots])
    for load in loads:
        load.wait()

    def both():
        return grads[...].reshape(2 * rows, depth)

    def unit(v, kind):
        return hidden[kind, :, :, :, :, width.cols(v)].reshape(rows, step)

    def crossed(which, v, products):
        value = products[:rows] * unit(v, 1).astype(F32) + products[rows:] * unit(v, 0).astype(F32)
        sums[which] += lanes(folded(value))

    def back(v):
        matrix(0, v).wait()
        matrix(1, v).wait()
        at = width.cols(v)
        weighted = against(both(), downs[at, :])
        moved = against(both(), alongs[at, :])
        width.put(v, 0, weighted[:rows])
        width.put(v, 1, weighted[rows:] + moved[:rows])
        width.mated(v).start()
        crossed(1, v, moved)

    def extra(v):
        matrix(2, v).wait()
        crossed(2, v, against(both(), befores[width.cols(v), :]))
        swapped = jnp.concatenate([unit(v, 1), unit(v, 0)])
        swap_gram[...] += against(swapped, swapped)

    def middle(v):
        grad_hidden, grad_hidden_dir = width.totals(v)
        cols = width.cols(v)
        gate_sum, up_sum, gate_dir, up_dir = (keeps[k, :, cols] for k in range(4))
        logistic = jax.nn.sigmoid(gate_sum)
        activation = gate_sum * logistic
        slope = logistic * (1.0 + gate_sum * (1.0 - logistic))
        curve = logistic * (1.0 - logistic) * (2.0 + gate_sum * (1.0 - 2.0 * logistic))
        grad_gate = (
            grad_hidden_dir * up_sum * slope + grad_hidden * up_dir * slope + grad_hidden * up_sum * curve * gate_dir
        ).astype(BF16)
        grad_up = (grad_hidden_dir * activation + grad_hidden * slope * gate_dir).astype(BF16)
        width.keep(v, 0, grad_gate)
        width.keep(v, 1, grad_up)
        width.spread(v)
        sums[1] += lanes(folded(grad_gate.astype(F32) * gate_dir + grad_up.astype(F32) * up_dir))

    def finish(v):
        width.complete(v)
        cols = width.cols(v)
        for kind in range(2):
            part = width.rows(v, kind)
            gram[...] += against(part, part)
            sums[2] += lanes(folded(part.astype(F32) * bx[kind, :, cols].astype(F32)))

    @pl.loop(0, steps + LAGS["done"])
    def _(i):
        staged(i, 0, steps, back)
        staged(i, LAGS["cross"], steps, width.cross)
        staged(i, LAGS["totals"], steps, middle)
        staged(i, LAGS["relay"], steps, width.relay)
        staged(i, LAGS["last"], steps, width.relay_last)
        staged(i, LAGS["done"], steps, finish)
        staged(i, LAGS["pair"], steps, width.pair)
        staged(i, LAGS["totals"], steps, extra)

    store = pltpu.make_async_copy(width.full, out_dirs, o_sem.at[0])
    store.start()
    every = tokens[...].reshape(rows, depth)
    sums[0] += lanes(folded(against(every, every) * gram[...])) + lanes(
        folded(against(both(), both()) * swap_gram[...])
    )
    shape = (1, 128)
    own = [jnp.full(shape, jnp.sum(sums[k])) for k in range(3)] + [jnp.full(shape, jnp.sum(norms[k])) for k in range(3)]
    for k in range(6):
        total_dp[k : k + 1] = own[k]
    total_dp[6:8] = jnp.zeros((2, 128), F32)
    dp_in[dp] = total_dp[...]

    first = [
        remote(total_dp, dp_in.at[dp], s1.at[i], r1.at[i], {"dp": spot}) for i, spot in enumerate(dp_spots)
    ]
    for copy in first:
        copy.start()
    for copy in first:
        copy.wait_recv()
    total = dp_in[0]
    for at in range(1, n):
        total = total + dp_in[at]
    tp_in[tp] = total
    second = [
        remote(tp_in.at[tp], tp_in.at[tp], s2.at[i], r2.at[i], {"tp": spot}) for i, spot in enumerate(tp_spots)
    ]
    for copy in second:
        copy.start()
    for copy in second:
        copy.wait_recv()
    total = tp_in[0]
    for at in range(1, t):
        total = total + tp_in[at]
    image_image, image_along, image_before = total[0:1], total[1:2], total[2:3]
    along_along, along_before, before_before = total[3:4], total[4:5], total[5:6]
    beta_old = beta_prev[0]
    alpha_coef = image_along / entries
    square = (
        image_image
        - 2.0 * alpha_coef * image_along
        - 2.0 * beta_old * image_before
        + alpha_coef * alpha_coef * along_along
        + 2.0 * alpha_coef * beta_old * along_before
        + beta_old * beta_old * before_before
    )
    beta_coef = jnp.sqrt(square / entries + 1e-06)
    inverse = 1.0 / beta_coef
    scales[0:1] = alpha_coef
    scales[1:2] = beta_coef
    scales[2:3] = inverse
    scales[3:4] = alpha_coef * inverse
    scales[4:5] = beta_old * inverse
    scales[5:8] = jnp.zeros((3, 128), F32)
    for copy in first + second:
        copy.wait_send()
    width.drain()
    store.wait()


def late(n, t, entries, tokens, units, keeps, grads, bx, norms, down, along, before, beta_prev):
    width, depth = down.shape
    rows = bx.shape[1]
    chunks = width // tile_of(width, max(128, width // 8))
    plan = Width(n, 1, chunks, 2, rows // n, width)
    small = (8, 128)
    return pl.pallas_call(
        functools.partial(late_kernel, n, t, entries, plan),
        out_shape=[jax.ShapeDtypeStruct(units.shape, BF16), jax.ShapeDtypeStruct(small, F32)],
        in_specs=[WHOLE] + [ANY] * 4 + [WHOLE] + [ANY] * 3 + [pl.BlockSpec(memory_space=pltpu.SMEM)],
        out_specs=[ANY, WHOLE],
        scratch_shapes=[
            VMEM(grads.shape, BF16),
            VMEM(units.shape, BF16),
            VMEM(keeps.shape, F32),
            VMEM(bx.shape, BF16),
            VMEM((width, depth), BF16),
            VMEM((width, depth), BF16),
            VMEM((width, depth), BF16),
            VMEM((3,) + small, F32),
            VMEM((rows, rows), F32),
            VMEM((2 * rows, 2 * rows), F32),
            VMEM((n,) + small, F32),
            VMEM(small, F32),
            VMEM((t,) + small, F32),
            DMA((4,)),
            DMA((3, chunks)),
            DMA((1,)),
            DMA((n - 1,)),
            DMA((n - 1,)),
            DMA((t - 1,)),
            DMA((t - 1,)),
        ]
        + plan.scratch(),
        compiler_params=pltpu.CompilerParams(collective_id=2, has_side_effects=True, vmem_limit_bytes=LIMIT),
    )(tokens, units, keeps, grads, bx, norms, down, along, before, beta_prev)


def transposed(one, two):
    return lax.dot_general(one, two, (((0,), (0,)), ((), ())), preferred_element_type=F32)


def next_kernel(scales, tokens, dirs, units, grads, along_gate, along_up, along_down, before_gate, before_up, before_down, out_gate, out_up, out_down, tall):
    inverse, alpha, beta = scales[2, 0], scales[3, 0], scales[4, 0]

    @pl.when(pl.program_id(0) == 0)
    def _():
        tall[...] = tokens[...].T

    def blend(image, along, before, out):
        out[...] = (image * inverse - along[...].astype(F32) * alpha - before[...].astype(F32) * beta).astype(BF16)

    blend(dot(tall[...], dirs[0]), along_gate, before_gate, out_gate)
    blend(dot(tall[...], dirs[1]), along_up, before_up, out_up)
    image = transposed(units[1], grads[0]) + transposed(units[0], grads[1])
    blend(image, along_down, before_down, out_down)


def next_parts(scales, tokens, dirs, units, grads, alongs, befores):
    rows, depth = tokens.shape
    width = dirs.shape[2]
    tile = tile_of(width, 256)
    wide = pl.BlockSpec((depth, tile), lambda i: (0, i))
    tall = pl.BlockSpec((tile, depth), lambda i: (i, 0))
    return pl.pallas_call(
        next_kernel,
        grid=(width // tile,),
        out_shape=[jax.ShapeDtypeStruct((depth, width), BF16)] * 2 + [jax.ShapeDtypeStruct((width, depth), BF16)],
        in_specs=[
            pl.BlockSpec(memory_space=pltpu.SMEM),
            pl.BlockSpec((rows, depth), lambda i: (0, 0)),
            pl.BlockSpec((2, rows, tile), lambda i: (0, 0, i)),
            pl.BlockSpec((2, rows, tile), lambda i: (0, 0, i)),
            pl.BlockSpec((2, rows, depth), lambda i: (0, 0, 0)),
        ]
        + [wide, wide, tall] * 2,
        out_specs=[wide, wide, tall],
        scratch_shapes=[VMEM((depth, rows), BF16)],
        compiler_params=pltpu.CompilerParams(vmem_limit_bytes=LIMIT),
    )(scales, tokens, dirs, units, grads, *alongs, *befores)


def on_device(
    n,
    t,
    tokens,
    targets,
    gate_weight,
    up_weight,
    down_weight,
    direction_gate,
    direction_up,
    direction_down,
    previous_gate,
    previous_up,
    previous_down,
    beta_prev,
):
    everyone, units, keeps, grads, bx, norms = early(
        n,
        t,
        tokens,
        targets,
        gate_weight,
        up_weight,
        down_weight,
        direction_gate,
        direction_up,
        direction_down,
        previous_gate,
        previous_up,
        previous_down,
    )
    entries = float(n * t * (gate_weight.size + up_weight.size + down_weight.size))
    dirs, scales = late(
        n, t, entries, everyone, units, keeps, grads, bx, norms, down_weight, direction_down, previous_down, beta_prev
    )
    rows, depth = bx.shape[1], tokens.shape[1]
    next_gate, next_up, next_down = next_parts(
        scales,
        everyone.reshape(rows, depth),
        dirs.reshape(bx.shape),
        units.reshape(bx.shape),
        grads.reshape(2, rows, depth),
        (direction_gate, direction_up, direction_down),
        (previous_gate, previous_up, previous_down),
    )
    return (next_gate, next_up, next_down, scales[:2, 0])


def solution(mesh):
    wide, tall = P("dp", "tp"), P("tp", "dp")
    in_specs = (tall, tall, wide, wide, tall, wide, wide, tall, wide, wide, tall, P())
    return jax.shard_map(
        functools.partial(on_device, mesh.shape["dp"], mesh.shape["tp"]),
        mesh=mesh,
        in_specs=in_specs,
        out_specs=(wide, wide, tall, P()),
        check_vma=False,
    )
```

```python
import functools

import jax
import jax.numpy as jnp
from jax import lax
from jax.experimental import pallas as pl
from jax.experimental.pallas import tpu as pltpu
from jax.sharding import PartitionSpec as P

MESH = pl.DeviceIdType.MESH
VMEM = pltpu.VMEM
DMA = pltpu.SemaphoreType.DMA
ANY = pl.BlockSpec(memory_space=pl.ANY)
WHOLE = pl.BlockSpec(memory_space=pltpu.VMEM)
F32 = jnp.float32
BF16 = jnp.bfloat16
LIMIT = 62 * 1024 * 1024
LATE = 24 * 1024 * 1024
LAST = LATE


def tile_of(size, most):
    tile = min(size, most)
    while size % tile:
        tile //= 2
    return tile


def dot(one, two):
    return jnp.dot(one, two, preferred_element_type=F32)


def against(one, two):
    return lax.dot_general(one, two, (((1,), (1,)), ((), ())), preferred_element_type=F32)


def greet(targets):
    barrier = pltpu.get_barrier_semaphore()
    for target in targets:
        pl.semaphore_signal(barrier, inc=1, device_id=target, device_id_type=MESH)
    pl.semaphore_wait(barrier, len(targets))


def remote(src, dst, send_sem, recv_sem, target):
    return pltpu.make_async_remote_copy(
        src_ref=src, dst_ref=dst, send_sem=send_sem, recv_sem=recv_sem, device_id=target, device_id_type=MESH
    )


def folded(values, width=None):
    rows, cols = values.shape
    return values.reshape(rows // 8, 8, cols).sum(axis=0)


def lanes(values):
    total = values[:, :128]
    for at in range(128, values.shape[1], 128):
        total = total + values[:, at : at + 128]
    return total


class Width:
    def __init__(self, n, phases, chunks, kinds, share, width):
        self.n, self.phases, self.chunks, self.kinds = n, phases, chunks, kinds
        self.share, self.width = share, width
        self.steps = phases * chunks
        self.ys, self.xs = 2, n // 4
        self.step = width // chunks
        self.slots = min(self.steps, 8)

    def scratch(self):
        p, y, x, share, width, v = self.phases, self.ys, self.xs, self.share, self.width, self.steps
        return [
            VMEM((p, 2, y, x, 2, share, width), BF16),
            VMEM((p, 2, y, x, share, width), BF16),
            VMEM((p, 2, y, x, share, width), BF16),
            VMEM((p, x, y, share, width), BF16),
            VMEM((p, x, share, width), BF16),
            VMEM((p, share, width), BF16),
            VMEM((p, x, share, width), BF16),
            VMEM((p, share, width), BF16),
            VMEM((p, x, share, width), BF16),
            VMEM((self.kinds, y, x, 2, share, width), BF16),
        ] + [
            DMA(shape)
            for one, slots in zip((1, x - 1, 1, 1, x - 1, x - 1, 1, x - 1, x - 1, 1), [self.slots] * 9 + [v])
            for shape in ((one,), (slots, one))
        ]

    def bind(self, refs):
        (self.x, self.mate_in, self.paired, self.x1, self.y1, self.y2, self.x2, self.sa, self.sb, self.full) = refs[:10]
        sems = refs[10:]
        self.sems = [(sems[i], sems[i + 1]) for i in range(0, len(sems), 2)]
        me = lax.axis_index("dp")
        self.core = lax.rem(me, 2)
        chip = lax.div(me, 2)
        self.px, self.py = lax.rem(chip, self.xs), lax.div(chip, self.xs)
        self.qy = 1 - self.py
        self.mate = self.at(self.py, self.px, 1 - self.core)
        self.across = self.at(self.qy, self.px, self.core)
        self.to = [lax.rem(self.px + s, self.xs) for s in range(self.xs)]
        self.off = [lax.rem(self.px + self.xs - s, self.xs) for s in range(self.xs)]

    def at(self, y, x, core):
        return {"dp": (y * self.xs + x) * 2 + core}

    def partners(self):
        row = [self.at(self.py, self.to[s], self.core) for s in range(1, self.xs)]
        return [self.mate, self.across] + row

    def cols(self, v, part=0, parts=1):
        size = self.step // parts
        start = lax.rem(v, self.chunks) * self.step + part * size
        return pl.ds(pl.multiple_of(start, size), size)

    def phase(self, v):
        return lax.div(v, self.chunks)

    def row(self, s):
        return self.at(self.py, self.to[s], self.core)

    def copy(self, which, src, dst, v, target, k=1):
        send, recv = self.sems[which]
        return remote(src, dst, send.at[k - 1], recv.at[lax.rem(v, recv.shape[0]), k - 1], target)

    def mated(self, v):
        p, cols = self.phase(v), self.cols(v)
        src = self.x.at[p, :, :, :, 1 - self.core, :, cols]
        return self.copy(0, src, self.mate_in.at[p, :, :, :, :, cols], v, self.mate)

    def first_x(self, v, k):
        p, cols = self.phase(v), self.cols(v)
        src = self.paired.at[p, 0, :, self.to[k], :, cols]
        return self.copy(1, src, self.x1.at[p, self.px, :, :, cols], v, self.row(k), k)

    def first_y(self, v):
        p, cols = self.phase(v), self.cols(v)
        return self.copy(2, self.paired.at[p, 1, self.qy, :, :, cols], self.y1.at[p, :, :, cols], v, self.across)

    def second_y(self, v):
        p, cols = self.phase(v), self.cols(v)
        return self.copy(3, self.sa.at[p, :, cols], self.y2.at[p, :, cols], v, self.across)

    def second_x(self, v, k):
        p, cols = self.phase(v), self.cols(v)
        return self.copy(4, self.sb.at[p, self.to[k], :, cols], self.x2.at[p, self.px, :, cols], v, self.row(k), k)

    def block(self, v, y, x):
        if self.phases > 1:
            return self.full.at[self.phase(v), y, x, self.core, :, self.cols(v)]
        return self.full.at[:, y, x, self.core, :, self.cols(v)]

    def half(self, v, y, x, part):
        if self.phases == 1:
            return self.full.at[part, y, x, self.core, :, self.cols(v)]
        if self.step % 256 == 0:
            return self.full.at[self.phase(v), y, x, self.core, :, self.cols(v, part, 2)]
        rows = pl.ds(part * (self.share // 2), self.share // 2)
        return self.full.at[self.phase(v), y, x, self.core, rows, self.cols(v)]

    def gather_x(self, v, k):
        mine = self.block(v, self.py, self.px)
        return self.copy(5, mine, mine, v, self.row(k), k)

    def gather_y(self, v):
        mine = self.block(v, self.py, self.px)
        return self.copy(6, mine, mine, v, self.across)

    def pass_y(self, v, k):
        piece = self.half(v, self.py, self.off[k], 0)
        return self.copy(7, piece, piece, v, self.across, k)

    def pass_x(self, v, k):
        piece = self.half(v, self.qy, self.px, 1)
        return self.copy(8, piece, piece, v, self.row(k), k)

    def hand(self, v, role):
        y, k = (self.py, role) if role < self.xs else (self.qy, role - self.xs)
        piece = self.block(v, y, self.off[k])
        return self.copy(9, piece, piece, v, self.mate)

    def handed(self, v):
        kinds = self.phase(v) if self.phases > 1 else slice(None)
        every = self.full.at[kinds, :, :, self.core, :, self.cols(v)]
        return self.copy(9, every, every, v, self.mate)

    def put(self, v, kind, rows):
        p, cols = self.phase(v), self.cols(v)
        shape = (self.ys, self.xs, 2, self.share, self.step)
        self.x[p, kind, :, :, :, :, cols] = rows.astype(BF16).reshape(shape)

    def pair(self, v):
        p, cols = self.phase(v), self.cols(v)
        self.mated(v).wait_recv()
        self.paired[p, :, :, :, :, cols] = (
            self.x[p, :, :, :, self.core, :, cols].astype(F32) + self.mate_in[p, :, :, :, :, cols].astype(F32)
        ).astype(BF16)
        for k in range(1, self.xs):
            self.first_x(v, k).start()
        self.first_y(v).start()

    def cross(self, v):
        p, cols = self.phase(v), self.cols(v)
        for k in range(1, self.xs):
            self.first_x(v, k).wait_recv()
        total = self.paired[p, 0, self.qy, self.px, :, cols].astype(F32)
        for k in range(1, self.xs):
            total = total + self.x1[p, self.off[k], self.qy, :, cols].astype(F32)
        self.sa[p, :, cols] = total.astype(BF16)
        self.second_y(v).start()
        self.first_y(v).wait_recv()
        for k in range(1, self.xs):
            total = self.paired[p, 1, self.py, self.to[k], :, cols].astype(F32) + self.y1[
                p, self.to[k], :, cols
            ].astype(F32)
            self.sb[p, self.to[k], :, cols] = total.astype(BF16)
            self.second_x(v, k).start()

    def totals(self, v):
        p, cols = self.phase(v), self.cols(v)
        self.second_y(v).wait_recv()
        for k in range(1, self.xs):
            self.second_x(v, k).wait_recv()
        one = self.paired[p, 0, self.py, self.px, :, cols].astype(F32) + self.y2[p, :, cols].astype(F32)
        two = self.paired[p, 1, self.py, self.px, :, cols].astype(F32) + self.y1[p, self.px, :, cols].astype(F32)
        for k in range(1, self.xs):
            one = one + self.x1[p, self.off[k], self.py, :, cols].astype(F32)
            two = two + self.x2[p, self.off[k], :, cols].astype(F32)
        return one, two

    def keep(self, v, kind, rows):
        self.full[kind, self.py, self.px, self.core, :, self.cols(v)] = rows.astype(BF16)

    def spread(self, v):
        for k in range(1, self.xs):
            self.gather_x(v, k).start()
        self.gather_y(v).start()
        self.hand(v, 0).start()

    def relay(self, v):
        for k in range(1, self.xs):
            self.gather_x(v, k).wait_recv()
            self.pass_y(v, k).start()
        self.gather_y(v).wait_recv()
        for k in range(1, self.xs):
            self.pass_x(v, k).start()
        for role in range(1, self.xs + 1):
            self.hand(v, role).start()

    def relay_last(self, v):
        for k in range(1, self.xs):
            self.pass_y(v, k).wait_recv()
            self.pass_x(v, k).wait_recv()
            self.hand(v, self.xs + k).start()

    def complete(self, v):
        self.handed(v).wait_recv()

    def rows(self, v, kind):
        cols = self.cols(v)
        return self.full[kind, :, :, :, :, cols].reshape(self.n * self.share, self.step)

    def drain(self):
        full = self.full
        mine, half = full.at[:, self.py, self.px, self.core], full.at[0, self.py, self.px, self.core]
        every = full.at[:, :, :, self.core]
        self.copy(0, self.x.at[:, :, :, :, 1 - self.core], self.mate_in, 0, self.mate).wait_send()
        self.copy(2, self.paired.at[:, 1, self.qy], self.y1, 0, self.across).wait_send()
        self.copy(3, self.sa, self.y2, 0, self.across).wait_send()
        self.copy(6, mine, mine, 0, self.across).wait_send()
        self.copy(9, every, every, 0, self.mate).wait_send()
        for k in range(1, self.xs):
            self.copy(1, self.paired.at[:, 0, :, self.to[k]], self.x1.at[:, self.px], 0, self.row(k), k).wait_send()
            self.copy(4, self.sb.at[:, self.to[k]], self.x2.at[:, self.px], 0, self.row(k), k).wait_send()
            self.copy(5, mine, mine, 0, self.row(k), k).wait_send()
            self.copy(7, half, half, 0, self.across, k).wait_send()
            self.copy(8, half, half, 0, self.row(k), k).wait_send()


LAGS = dict(pair=1, cross=3, unit=3, totals=5, relay=7, last=9, done=10)


def staged(i, lag, steps, body):
    v = i - lag

    @pl.when((v >= 0) & (v < steps))
    def _():
        body(v)


DEEP = 4
SLOTS = 3


def squares(along_ref, before_ref, norms):
    rows, width = along_ref.shape
    step = tile_of(rows, 32)

    def body(i, sums):
        at = pl.ds(pl.multiple_of(i * step, step), step)
        along = along_ref[at, :].astype(F32)
        before = before_ref[at, :].astype(F32)
        products = (along * along, along * before, before * before)
        return tuple(have + folded(product) for have, product in zip(sums, products))

    zero = jnp.zeros((8, width), F32)
    sums = lax.fori_loop(0, rows // step, body, (zero, zero, zero))
    for kind in range(3):
        norms[kind] += lanes(sums[kind])


def early_kernel(n, t, width, *refs):
    (tokens, targets, gate, up, down, along_gate, along_up, along_down, before_gate, before_up, before_down) = refs[:11]
    (out_tokens, out_units, out_keeps, out_grads, out_before, norms) = refs[11:17]
    (tok, keeps, bx, weights, downs, alongs, wide, tall, acc, zx, zin, gz) = refs[17:29]
    (tok_s, tok_r, w_sem, d_sem, wide_sem, tall_sem, zs, zr, gs, gr, o_sem) = refs[29:40]
    width.bind(refs[40:])
    chunks, steps, step = width.chunks, width.steps, width.step
    share, depth = tokens.shape
    rows = t * share
    me = lax.axis_index("tp")
    spots = [lax.rem(me + s, t) for s in range(1, t)]
    sources = [lax.rem(me + t - s, t) for s in range(1, t)]

    def col(v):
        return width.cols(v)

    def load(v, one, two, start):
        slot = lax.rem(v, DEEP)
        for kind, ref in enumerate((one, two)):
            copy = pltpu.make_async_copy(ref.at[:, col(v)], weights.at[slot, kind], w_sem.at[slot, kind])
            if start:
                copy.start()
            else:
                copy.wait()

    def fetch(v):
        @pl.when(v < chunks)
        def _():
            load(v, gate, up, True)

        @pl.when((v >= chunks) & (v < steps))
        def _():
            load(v, along_gate, along_up, True)

    for v in range(DEEP):
        fetch(jnp.int32(v))

    def wide_copies(one, two, c):
        slot = lax.rem(c, SLOTS)
        return [
            pltpu.make_async_copy(ref.at[:, col(c)], wide.at[slot, kind], wide_sem.at[slot, kind])
            for kind, ref in enumerate((one, two))
            if ref is not None
        ]

    def tall_copies(c):
        slot = lax.rem(c, SLOTS)
        return [
            pltpu.make_async_copy(ref.at[col(c), :], tall.at[slot, kind], tall_sem.at[slot, kind])
            for kind, ref in enumerate((along_down, before_down))
        ]

    def open_stream(copies):
        for c in range(min(SLOTS, chunks)):
            for copy in copies(jnp.int32(c)):
                copy.start()

    def turn(copies, c, body):
        for copy in copies(c):
            copy.wait()
        body(c, lax.rem(c, SLOTS))

        @pl.when(c + SLOTS < chunks)
        def _():
            for copy in copies(c + SLOTS):
                copy.start()

    def run_stream(copies, body):
        @pl.loop(0, chunks)
        def _(c):
            turn(copies, c, body)

    gate_stream = functools.partial(wide_copies, along_gate, before_gate)
    up_stream = functools.partial(wide_copies, along_up, before_up)
    again_stream = functools.partial(wide_copies, None, before_gate)
    open_stream(gate_stream)
    load_down = pltpu.make_async_copy(down, downs, d_sem.at[0])
    load_along = pltpu.make_async_copy(along_down, alongs, d_sem.at[1])

    norms[...] = jnp.zeros_like(norms)
    greet(width.partners() + [{"tp": spot} for spot in spots])

    def gather(i):
        return remote(tokens, tok.at[me], tok_s.at[i], tok_r.at[i], {"tp": spots[i]})

    for i in range(t - 1):
        gather(i).start()
    tok[me] = tokens[...]

    def norm_wide(c, slot):
        squares(wide.at[slot, 0], wide.at[slot, 1], norms)

    run_stream(gate_stream, norm_wide)
    open_stream(up_stream)
    for i in range(t - 1):
        gather(i).wait_recv()

    def everyone():
        return tok[...].reshape(rows, depth)

    acc[...] = jnp.zeros_like(acc)

    def front(v):
        load(v, gate, up, False)
        slot = lax.rem(v, DEEP)
        for kind in range(2):
            width.put(v, kind, dot(everyone(), weights[slot, kind]))
        width.mated(v).start()
        fetch(v + DEEP)

    def sums(v):
        one, two = width.totals(v)
        cols = col(v)
        p = width.phase(v)

        @pl.when(p == 0)
        def _():
            keeps[0, :, cols] = one
            keeps[1, :, cols] = two
            width.keep(v, 0, one * jax.nn.sigmoid(one) * two)

        @pl.when(p == 1)
        def _():
            keeps[2, :, cols] = one
            keeps[3, :, cols] = two
            gate_sum, up_sum = keeps[0, :, cols], keeps[1, :, cols]
            logistic = jax.nn.sigmoid(gate_sum)
            slope = logistic * (1.0 + gate_sum * (1.0 - logistic))
            width.keep(v, 1, slope * up_sum * one + gate_sum * logistic * two)

        width.spread(v)

    def middle(v):
        width.complete(v)
        p, at = width.phase(v), col(v)

        @pl.when(v == 0)
        def _():
            load_down.wait()

        @pl.when(v == chunks)
        def _():
            load_along.wait()

        @pl.when(p == 0)
        def _():
            acc[0] += dot(width.rows(v, 0), downs[at, :])

        @pl.when(p == 1)
        def _():
            acc[1] += dot(width.rows(v, 1), downs[at, :]) + dot(width.rows(v, 0), alongs[at, :])

    def z_first(p, i):
        return remote(zx.at[p, spots[i]], zin.at[p, me], zs.at[p, i], zr.at[p, i], {"tp": spots[i]})

    def z_second(p, i):
        return remote(gz.at[p, me], gz.at[p, me], gs.at[p, i], gr.at[p, i], {"tp": spots[i]})

    def z_send(p):
        zx[p] = acc[p].astype(BF16).reshape(t, share, depth)
        for i in range(t - 1):
            z_first(p, i).start()

    def z_finish(p):
        for i in range(t - 1):
            z_first(p, i).wait_recv()
        total = zx[p, me].astype(F32)
        for at in sources:
            total = total + zin[p, at].astype(F32)
        if p == 0:
            total = total - targets[...].astype(F32)
        gz[p, me] = (total / rows).astype(BF16)
        for i in range(t - 1):
            z_second(p, i).start()

    def before_of(kind):
        def body(c, slot):
            bx[kind, :, col(c)] = dot(everyone(), wide[slot, 1]).astype(BF16)

        return body

    def norm_and_before(c, slot):
        norm_wide(c, slot)
        before_of(1)(c, slot)

    def norm_tall(c, slot):
        squares(tall.at[slot, 0], tall.at[slot, 1], norms)

    def unit(v):
        @pl.when(v < chunks)
        def _():
            turn(up_stream, v, norm_and_before)

        @pl.when(v >= chunks)
        def _():
            turn(tall_copies, v - chunks, norm_tall)

    ready = chunks - 1 + LAGS["done"]
    last = steps + LAGS["done"]
    settle = min(ready + 4, last - 1)

    @pl.loop(0, last)
    def _(i):
        staged(i, 0, steps, front)
        staged(i, LAGS["unit"], steps, unit)
        staged(i, LAGS["cross"], steps, width.cross)
        staged(i, LAGS["totals"], steps, sums)
        staged(i, LAGS["relay"], steps, width.relay)
        staged(i, LAGS["last"], steps, width.relay_last)
        staged(i, LAGS["done"], steps, middle)
        staged(i, LAGS["pair"], steps, width.pair)

        @pl.when(i == min(4, ready))
        def _():
            load_down.start()

        @pl.when(i == min(7, ready))
        def _():
            open_stream(tall_copies)

        @pl.when(i == min(11, ready))
        def _():
            load_along.start()

        @pl.when(i == ready)
        def _():
            z_send(0)

        @pl.when(i == settle)
        def _():
            z_finish(0)

    z_send(1)
    open_stream(again_stream)

    stores = [
        pltpu.make_async_copy(tok, out_tokens, o_sem.at[0]),
        pltpu.make_async_copy(width.full, out_units, o_sem.at[1]),
        pltpu.make_async_copy(keeps, out_keeps, o_sem.at[2]),
    ]
    for store in stores:
        store.start()
    run_stream(again_stream, before_of(0))
    stores.append(pltpu.make_async_copy(bx, out_before, o_sem.at[3]))
    stores[-1].start()
    z_finish(1)

    for p in range(2):
        for i in range(t - 1):
            z_second(p, i).wait_recv()
    stores.append(pltpu.make_async_copy(gz, out_grads, o_sem.at[4]))
    stores[-1].start()
    for i in range(t - 1):
        gather(i).wait_send()
        for p in range(2):
            z_first(p, i).wait_send()
            z_second(p, i).wait_send()
    width.drain()
    for store in stores:
        store.wait()


def early(n, t, tokens, targets, gate, up, down, along_gate, along_up, along_down, before_gate, before_up, before_down):
    share, depth = tokens.shape
    width = gate.shape[1]
    rows = t * share
    chunks = width // tile_of(width, max(128, width // 8))
    plan = Width(n, 2, chunks, 2, rows // n, width)
    step = plan.step
    keeps = (4, plan.share, width)
    units = (2, plan.ys, plan.xs, 2, plan.share, width)
    z = (2, t, share, depth)
    return pl.pallas_call(
        functools.partial(early_kernel, n, t, plan),
        out_shape=[
            jax.ShapeDtypeStruct((t, share, depth), BF16),
            jax.ShapeDtypeStruct(units, BF16),
            jax.ShapeDtypeStruct(keeps, F32),
            jax.ShapeDtypeStruct(z, BF16),
            jax.ShapeDtypeStruct((2, rows, width), BF16),
            jax.ShapeDtypeStruct((3, 8, 128), F32),
        ],
        in_specs=[WHOLE, WHOLE] + [ANY] * 9,
        out_specs=[ANY] * 5 + [WHOLE],
        scratch_shapes=[
            VMEM((t, share, depth), BF16),
            VMEM(keeps, F32),
            VMEM((2, rows, width), BF16),
            VMEM((DEEP, 2, depth, step), BF16),
            VMEM((width, depth), BF16),
            VMEM((width, depth), BF16),
            VMEM((SLOTS, 2, depth, step), BF16),
            VMEM((SLOTS, 2, step, depth), BF16),
            VMEM((2, rows, depth), F32),
            VMEM(z, BF16),
            VMEM(z, BF16),
            VMEM(z, BF16),
            DMA((t - 1,)),
            DMA((t - 1,)),
            DMA((DEEP, 2)),
            DMA((2,)),
            DMA((SLOTS, 2)),
            DMA((SLOTS, 2)),
            DMA((2, t - 1)),
            DMA((2, t - 1)),
            DMA((2, t - 1)),
            DMA((2, t - 1)),
            DMA((5,)),
        ]
        + plan.scratch(),
        compiler_params=pltpu.CompilerParams(collective_id=1, has_side_effects=True, vmem_limit_bytes=LIMIT),
    )(tokens, targets, gate, up, down, along_gate, along_up, along_down, before_gate, before_up, before_down)


def late_kernel(n, t, entries, width, *refs):
    (tokens, units, keeps_in, grads_in, before_in, norms, down, along, before) = refs[:9]
    wide_in, beta_prev, out_dirs, scales, alongs, wide_out = refs[9:12], refs[12], refs[13], refs[14], refs[15], refs[16:19]
    (grads, hidden, keeps, bx, downs, befores, sums, gram, swap_gram, dp_in, total_dp, tp_in) = refs[19:31]
    (in_sem, m_sem, w_sem, o_sem, s1, r1, s2, r2) = refs[31:39]
    width.bind(refs[39:])
    chunks, steps, step = width.chunks, width.steps, width.step
    depth = down.shape[1]
    rows = n * width.share
    dp, tp = lax.axis_index("dp"), lax.axis_index("tp")
    dp_spots = [lax.rem(dp + s, n) for s in range(1, n)]
    tp_spots = [lax.rem(tp + s, t) for s in range(1, t)]

    loads = [
        pltpu.make_async_copy(src, dst, in_sem.at[i])
        for i, (src, dst) in enumerate(((grads_in, grads), (units, hidden), (keeps_in, keeps), (before_in, bx)))
    ]

    def matrix(which, c):
        at, slot = width.cols(c), lax.rem(c, DEEP)
        src = (down, along, before)[which].at[at, :]
        dst = alongs.at[at, :] if which == 1 else (downs, befores)[which // 2].at[slot]
        return pltpu.make_async_copy(src, dst, m_sem.at[which, slot])

    def fetch(c):
        @pl.when(c < steps)
        def _():
            for which in range(3):
                matrix(which, c).start()

    def ahead(c):
        for src, dst, sem in zip(wide_in, wide_out, range(3)):
            at = width.cols(c)
            pltpu.make_async_copy(src.at[:, at], dst.at[:, at], w_sem.at[sem]).start()

    for load in loads:
        load.start()
    for c in range(2):
        fetch(jnp.int32(c))
    sums[...] = jnp.zeros_like(sums)
    gram[...] = jnp.zeros_like(gram)
    swap_gram[...] = jnp.zeros_like(swap_gram)
    greet([{"dp": spot} for spot in dp_spots] + [{"tp": spot} for spot in tp_spots])
    loads[0].wait()
    for c in range(2, DEEP - 1):
        fetch(jnp.int32(c))
    for load in loads[1:]:
        load.wait()

    def both():
        return grads[...].reshape(2 * rows, depth)

    def unit(v, kind):
        return hidden[kind, :, :, :, :, width.cols(v)].reshape(rows, step)

    def crossed(which, v, products):
        value = products[:rows] * unit(v, 1).astype(F32) + products[rows:] * unit(v, 0).astype(F32)
        sums[which] += lanes(folded(value))

    def back(v):
        matrix(0, v).wait()
        matrix(1, v).wait()
        at = width.cols(v)
        weighted = against(both(), downs[lax.rem(v, DEEP)])
        moved = against(both(), alongs[at, :])
        width.put(v, 0, weighted[:rows])
        width.put(v, 1, weighted[rows:] + moved[:rows])
        width.mated(v).start()
        crossed(1, v, moved)
        fetch(v + DEEP - 1)

    def extra(v):
        matrix(2, v).wait()
        crossed(2, v, against(both(), befores[lax.rem(v, DEEP)]))
        swapped = jnp.concatenate([unit(v, 1), unit(v, 0)])
        swap_gram[...] += against(swapped, swapped)

    def middle(v):
        grad_hidden, grad_hidden_dir = width.totals(v)
        cols = width.cols(v)
        gate_sum, up_sum, gate_dir, up_dir = (keeps[k, :, cols] for k in range(4))
        logistic = jax.nn.sigmoid(gate_sum)
        activation = gate_sum * logistic
        slope = logistic * (1.0 + gate_sum * (1.0 - logistic))
        curve = logistic * (1.0 - logistic) * (2.0 + gate_sum * (1.0 - 2.0 * logistic))
        grad_gate = (
            grad_hidden_dir * up_sum * slope + grad_hidden * up_dir * slope + grad_hidden * up_sum * curve * gate_dir
        ).astype(BF16)
        grad_up = (grad_hidden_dir * activation + grad_hidden * slope * gate_dir).astype(BF16)
        width.keep(v, 0, grad_gate)
        width.keep(v, 1, grad_up)
        width.spread(v)
        sums[1] += lanes(folded(grad_gate.astype(F32) * gate_dir + grad_up.astype(F32) * up_dir))

    def finish(v):
        width.complete(v)
        cols = width.cols(v)
        for kind in range(2):
            part = width.rows(v, kind)
            gram[...] += against(part, part)
            sums[2] += lanes(folded(part.astype(F32) * bx[kind, :, cols].astype(F32)))

    @pl.loop(0, steps + LAGS["done"])
    def _(i):
        staged(i, 1, steps, extra)
        staged(i, 0, steps, back)
        staged(i, LAGS["cross"], steps, width.cross)
        staged(i, LAGS["totals"], steps, middle)
        staged(i, LAGS["relay"], steps, width.relay)
        staged(i, LAGS["last"], steps, width.relay_last)
        staged(i, LAGS["done"], steps, finish)
        staged(i, LAGS["pair"], steps, width.pair)
        staged(i, 6, steps, ahead)

    store = pltpu.make_async_copy(width.full, out_dirs, o_sem.at[0])
    store.start()
    every = tokens[...].reshape(rows, depth)
    sums[0] += lanes(folded(against(every, every) * gram[...])) + lanes(
        folded(against(both(), both()) * swap_gram[...])
    )
    shape = (1, 128)
    own = [jnp.full(shape, jnp.sum(sums[k])) for k in range(3)] + [jnp.full(shape, jnp.sum(norms[k])) for k in range(3)]
    for k in range(6):
        total_dp[k : k + 1] = own[k]
    total_dp[6:8] = jnp.zeros((2, 128), F32)
    dp_in[dp] = total_dp[...]

    first = [
        remote(total_dp, dp_in.at[dp], s1.at[i], r1.at[i], {"dp": spot}) for i, spot in enumerate(dp_spots)
    ]
    for copy in first:
        copy.start()
    for copy in first:
        copy.wait_recv()
    total = dp_in[0]
    for at in range(1, n):
        total = total + dp_in[at]
    tp_in[tp] = total
    second = [
        remote(tp_in.at[tp], tp_in.at[tp], s2.at[i], r2.at[i], {"tp": spot}) for i, spot in enumerate(tp_spots)
    ]
    for copy in second:
        copy.start()
    for copy in second:
        copy.wait_recv()
    total = tp_in[0]
    for at in range(1, t):
        total = total + tp_in[at]
    image_image, image_along, image_before = total[0:1], total[1:2], total[2:3]
    along_along, along_before, before_before = total[3:4], total[4:5], total[5:6]
    beta_old = beta_prev[0]
    alpha_coef = image_along / entries
    square = (
        image_image
        - 2.0 * alpha_coef * image_along
        - 2.0 * beta_old * image_before
        + alpha_coef * alpha_coef * along_along
        + 2.0 * alpha_coef * beta_old * along_before
        + beta_old * beta_old * before_before
    )
    beta_coef = jnp.sqrt(square / entries + 1e-06)
    inverse = 1.0 / beta_coef
    scales[0:1] = alpha_coef
    scales[1:2] = beta_coef
    scales[2:3] = inverse
    scales[3:4] = alpha_coef * inverse
    scales[4:5] = beta_old * inverse
    scales[5:8] = jnp.zeros((3, 128), F32)
    for copy in first + second:
        copy.wait_send()
    width.drain()
    store.wait()
    for src, dst, sem in zip(wide_in, wide_out, range(3)):
        pltpu.make_async_copy(src, dst, w_sem.at[sem]).wait()


def late(n, t, entries, tokens, units, keeps, grads, bx, norms, down, along, before, wides, beta_prev):
    width, depth = down.shape
    rows = bx.shape[1]
    chunks = width // tile_of(width, max(128, width // 8))
    plan = Width(n, 1, chunks, 2, rows // n, width)
    small = (8, 128)
    return pl.pallas_call(
        functools.partial(late_kernel, n, t, entries, plan),
        out_shape=[jax.ShapeDtypeStruct(units.shape, BF16), jax.ShapeDtypeStruct(small, F32)]
        + [VMEM(like.shape, BF16) for like in (along,) + wides],
        in_specs=[WHOLE] + [ANY] * 4 + [WHOLE] + [ANY] * 6 + [pl.BlockSpec(memory_space=pltpu.SMEM)],
        out_specs=[ANY] + [WHOLE] * 5,
        scratch_shapes=[
            VMEM(grads.shape, BF16),
            VMEM(units.shape, BF16),
            VMEM(keeps.shape, F32),
            VMEM(bx.shape, BF16),
            VMEM((DEEP, plan.step, depth), BF16),
            VMEM((DEEP, plan.step, depth), BF16),
            VMEM((3,) + small, F32),
            VMEM((rows, rows), F32),
            VMEM((2 * rows, 2 * rows), F32),
            VMEM((n,) + small, F32),
            VMEM(small, F32),
            VMEM((t,) + small, F32),
            DMA((4,)),
            DMA((3, DEEP)),
            DMA((3,)),
            DMA((1,)),
            DMA((n - 1,)),
            DMA((n - 1,)),
            DMA((t - 1,)),
            DMA((t - 1,)),
        ]
        + plan.scratch(),
        compiler_params=pltpu.CompilerParams(collective_id=2, has_side_effects=True, vmem_limit_bytes=LATE),
    )(tokens, units, keeps, grads, bx, norms, down, along, before, *wides, beta_prev)


def next_kernel(scales, tokens, dirs, units, grads, before_up, before_down, along_down, along_gate, along_up, before_gate, *refs):
    out_gate, out_up, out_down, coefs, tok, tall, ways, hidden, slopes, ups, downs, wides, talls, in_sem, b_sem, o_sem = refs
    inverse, alpha, beta = scales[2, 0], scales[3, 0], scales[4, 0]
    depth, width = along_gate.shape
    rows = tokens.shape[0]
    tile, part = wides.shape[2], tile_of(depth, 256)
    count = width // tile
    loads = [
        pltpu.make_async_copy(src, dst, in_sem.at[i])
        for i, (src, dst) in enumerate(
            ((tokens, tok), (dirs.at[0], ways.at[0]), (dirs.at[1], ways.at[1]), (units, hidden), (grads, slopes))
        )
    ]
    for load in loads:
        load.start()

    def piece(j):
        return pl.ds(pl.multiple_of(j * tile, tile), tile)

    def previous(which, j):
        slot = lax.rem(j, DEEP)
        src, dst = ((before_up.at[:, piece(j)], ups), (before_down.at[piece(j), :], downs))[which]
        return pltpu.make_async_copy(src, dst.at[slot], b_sem.at[which, slot])

    for which in range(2):
        for j in range(min(DEEP, count)):
            previous(which, jnp.int32(j)).start()
    coefs[0] = scales[0, 0]
    coefs[1] = scales[1, 0]

    def blend(image, along, before):
        return (image * inverse - along.astype(F32) * alpha - before.astype(F32) * beta).astype(BF16)

    def store(which, j):
        slot = lax.rem(j, DEEP)
        if which < 2:
            dst, src = (out_gate, out_up)[which].at[:, piece(j)], wides.at[slot]
        else:
            dst, src = out_down.at[piece(j), :], talls.at[slot]
        return pltpu.make_async_copy(src, dst, o_sem.at[min(which, 2) // 2, slot])

    loads[0].wait()
    tall[...] = tok[...].T
    for which, along in enumerate((along_gate, along_up)):
        loads[1 + which].wait()

        @pl.loop(0, count)
        def _(j):
            slot, cols = lax.rem(j, DEEP), piece(j)
            if which == 0:
                @pl.when(j >= DEEP)
                def _():
                    store(0, j).wait()
            else:
                previous(0, j).wait()
                store(0, j).wait()
            way = ways[which, :, cols]
            for at in range(0, depth, part):
                here = slice(at, at + part)
                before = ups[slot, here, :] if which else before_gate[here, cols]
                wides[slot, here, :] = blend(dot(tall[here, :], way), along[here, cols], before)
            store(which, j).start()
            if which:
                @pl.when(j + DEEP < count)
                def _():
                    previous(0, j + DEEP).start()

    loads[3].wait()
    loads[4].wait()

    @pl.loop(0, count)
    def _(j):
        slot, cols = lax.rem(j, DEEP), piece(j)

        @pl.when(j >= DEEP)
        def _():
            store(2, j).wait()

        previous(1, j).wait()
        swapped = jnp.concatenate([hidden[1, :, cols], hidden[0, :, cols]]).T
        for at in range(0, depth, part):
            here = slice(at, at + part)
            both = slopes[:, :, here].reshape(2 * rows, part)
            talls[slot, :, here] = blend(dot(swapped, both), along_down[cols, here], downs[slot, :, here])
        store(2, j).start()

        @pl.when(j + DEEP < count)
        def _():
            previous(1, j + DEEP).start()

    for j in range(min(DEEP, count)):
        store(0, jnp.int32(j)).wait()
        store(2, jnp.int32(j)).wait()


def next_parts(scales, tokens, dirs, units, grads, before_up, before_down, *held):
    rows, depth = tokens.shape
    width = dirs.shape[2]
    tile = tile_of(width, max(128, min(256, width // DEEP)))
    smem = pl.BlockSpec(memory_space=pltpu.SMEM)
    return pl.pallas_call(
        next_kernel,
        out_shape=[jax.ShapeDtypeStruct((depth, width), BF16)] * 2
        + [jax.ShapeDtypeStruct((width, depth), BF16), jax.ShapeDtypeStruct((2,), F32)],
        in_specs=[smem] + [ANY] * 6 + [WHOLE] * 4,
        out_specs=[ANY] * 3 + [smem],
        scratch_shapes=[
            VMEM((rows, depth), BF16),
            VMEM((depth, rows), BF16),
            VMEM(dirs.shape, BF16),
            VMEM(dirs.shape, BF16),
            VMEM(grads.shape, BF16),
            VMEM((DEEP, depth, tile), BF16),
            VMEM((DEEP, tile, depth), BF16),
            VMEM((DEEP, depth, tile), BF16),
            VMEM((DEEP, tile, depth), BF16),
            DMA((5,)),
            DMA((2, DEEP)),
            DMA((2, DEEP)),
        ],
        compiler_params=pltpu.CompilerParams(vmem_limit_bytes=LAST),
    )(scales, tokens, dirs, units, grads, before_up, before_down, *held)


def on_device(
    n,
    t,
    tokens,
    targets,
    gate_weight,
    up_weight,
    down_weight,
    direction_gate,
    direction_up,
    direction_down,
    previous_gate,
    previous_up,
    previous_down,
    beta_prev,
):
    everyone, units, keeps, grads, bx, norms = early(
        n,
        t,
        tokens,
        targets,
        gate_weight,
        up_weight,
        down_weight,
        direction_gate,
        direction_up,
        direction_down,
        previous_gate,
        previous_up,
        previous_down,
    )
    entries = float(n * t * (gate_weight.size + up_weight.size + down_weight.size))
    wides = (direction_gate, direction_up, previous_gate)
    dirs, scales, *held = late(
        n, t, entries, everyone, units, keeps, grads, bx, norms, down_weight, direction_down, previous_down, wides, beta_prev
    )
    held = [pltpu.with_memory_space_constraint(array, VMEM) for array in held]
    rows, depth = bx.shape[1], tokens.shape[1]
    return tuple(next_parts(
        scales,
        everyone.reshape(rows, depth),
        dirs.reshape(bx.shape),
        units.reshape(bx.shape),
        grads.reshape(2, rows, depth),
        previous_up,
        previous_down,
        *held,
    ))


def solution(mesh):
    wide, tall = P("dp", "tp"), P("tp", "dp")
    in_specs = (tall, tall, wide, wide, tall, wide, wide, tall, wide, wide, tall, P())
    return jax.shard_map(
        functools.partial(on_device, mesh.shape["dp"], mesh.shape["tp"]),
        mesh=mesh,
        in_specs=in_specs,
        out_specs=(wide, wide, tall, P()),
        check_vma=False,
    )
```

```python
import functools

import jax
import jax.numpy as jnp
from jax import lax
from jax.experimental import pallas as pl
from jax.experimental.pallas import tpu as pltpu
from jax.sharding import PartitionSpec as P

MESH = pl.DeviceIdType.MESH
VMEM = pltpu.VMEM
DMA = pltpu.SemaphoreType.DMA
ANY = pl.BlockSpec(memory_space=pl.ANY)
WHOLE = pl.BlockSpec(memory_space=pltpu.VMEM)
F32 = jnp.float32
BF16 = jnp.bfloat16
LIMIT = 62 * 1024 * 1024
LATE = 22 * 1024 * 1024
LAST = LATE


def tile_of(size, most):
    tile = min(size, most)
    while size % tile:
        tile //= 2
    return tile


def dot(one, two):
    return jnp.dot(one, two, preferred_element_type=F32)


def against(one, two):
    return lax.dot_general(one, two, (((1,), (1,)), ((), ())), preferred_element_type=F32)


def greet(targets):
    barrier = pltpu.get_barrier_semaphore()
    for target in targets:
        pl.semaphore_signal(barrier, inc=1, device_id=target, device_id_type=MESH)
    pl.semaphore_wait(barrier, len(targets))


def remote(src, dst, send_sem, recv_sem, target):
    return pltpu.make_async_remote_copy(
        src_ref=src, dst_ref=dst, send_sem=send_sem, recv_sem=recv_sem, device_id=target, device_id_type=MESH
    )


def folded(values, width=None):
    rows, cols = values.shape
    return values.reshape(rows // 8, 8, cols).sum(axis=0)


def lanes(values):
    total = values[:, :128]
    for at in range(128, values.shape[1], 128):
        total = total + values[:, at : at + 128]
    return total


class Width:
    def __init__(self, n, phases, chunks, kinds, share, width):
        self.n, self.phases, self.chunks, self.kinds = n, phases, chunks, kinds
        self.share, self.width = share, width
        self.steps = phases * chunks
        self.ys, self.xs = 2, n // 4
        self.step = width // chunks
        self.slots = min(self.steps, 8)

    def scratch(self):
        p, y, x, share, width, v = self.phases, self.ys, self.xs, self.share, self.width, self.steps
        return [
            VMEM((p, 2, y, x, 2, share, width), BF16),
            VMEM((p, 2, y, x, share, width), BF16),
            VMEM((p, 2, y, x, share, width), BF16),
            VMEM((p, x, y, share, width), BF16),
            VMEM((p, x, share, width), BF16),
            VMEM((p, share, width), BF16),
            VMEM((p, x, share, width), BF16),
            VMEM((p, share, width), BF16),
            VMEM((p, x, share, width), BF16),
            VMEM((self.kinds, y, x, 2, share, width), BF16),
        ] + [
            DMA(shape)
            for one, slots in zip((1, x - 1, 1, 1, x - 1, x - 1, 1, x - 1, x - 1, 1), [self.slots] * 9 + [v])
            for shape in ((one,), (slots, one))
        ]

    def bind(self, refs):
        (self.x, self.mate_in, self.paired, self.x1, self.y1, self.y2, self.x2, self.sa, self.sb, self.full) = refs[:10]
        sems = refs[10:]
        self.sems = [(sems[i], sems[i + 1]) for i in range(0, len(sems), 2)]
        me = lax.axis_index("dp")
        self.core = lax.rem(me, 2)
        chip = lax.div(me, 2)
        self.px, self.py = lax.rem(chip, self.xs), lax.div(chip, self.xs)
        self.qy = 1 - self.py
        self.mate = self.at(self.py, self.px, 1 - self.core)
        self.across = self.at(self.qy, self.px, self.core)
        self.to = [lax.rem(self.px + s, self.xs) for s in range(self.xs)]
        self.off = [lax.rem(self.px + self.xs - s, self.xs) for s in range(self.xs)]

    def at(self, y, x, core):
        return {"dp": (y * self.xs + x) * 2 + core}

    def partners(self):
        row = [self.at(self.py, self.to[s], self.core) for s in range(1, self.xs)]
        return [self.mate, self.across] + row

    def cols(self, v, part=0, parts=1):
        size = self.step // parts
        start = lax.rem(v, self.chunks) * self.step + part * size
        return pl.ds(pl.multiple_of(start, size), size)

    def phase(self, v):
        return lax.div(v, self.chunks)

    def row(self, s):
        return self.at(self.py, self.to[s], self.core)

    def copy(self, which, src, dst, v, target, k=1):
        send, recv = self.sems[which]
        return remote(src, dst, send.at[k - 1], recv.at[lax.rem(v, recv.shape[0]), k - 1], target)

    def mated(self, v):
        p, cols = self.phase(v), self.cols(v)
        src = self.x.at[p, :, :, :, 1 - self.core, :, cols]
        return self.copy(0, src, self.mate_in.at[p, :, :, :, :, cols], v, self.mate)

    def first_x(self, v, k):
        p, cols = self.phase(v), self.cols(v)
        src = self.paired.at[p, 0, :, self.to[k], :, cols]
        return self.copy(1, src, self.x1.at[p, self.px, :, :, cols], v, self.row(k), k)

    def first_y(self, v):
        p, cols = self.phase(v), self.cols(v)
        return self.copy(2, self.paired.at[p, 1, self.qy, :, :, cols], self.y1.at[p, :, :, cols], v, self.across)

    def second_y(self, v):
        p, cols = self.phase(v), self.cols(v)
        return self.copy(3, self.sa.at[p, :, cols], self.y2.at[p, :, cols], v, self.across)

    def second_x(self, v, k):
        p, cols = self.phase(v), self.cols(v)
        return self.copy(4, self.sb.at[p, self.to[k], :, cols], self.x2.at[p, self.px, :, cols], v, self.row(k), k)

    def block(self, v, y, x):
        if self.phases > 1:
            return self.full.at[self.phase(v), y, x, self.core, :, self.cols(v)]
        return self.full.at[:, y, x, self.core, :, self.cols(v)]

    def half(self, v, y, x, part):
        if self.phases == 1:
            return self.full.at[part, y, x, self.core, :, self.cols(v)]
        if self.step % 256 == 0:
            return self.full.at[self.phase(v), y, x, self.core, :, self.cols(v, part, 2)]
        rows = pl.ds(part * (self.share // 2), self.share // 2)
        return self.full.at[self.phase(v), y, x, self.core, rows, self.cols(v)]

    def gather_x(self, v, k):
        mine = self.block(v, self.py, self.px)
        return self.copy(5, mine, mine, v, self.row(k), k)

    def gather_y(self, v):
        mine = self.block(v, self.py, self.px)
        return self.copy(6, mine, mine, v, self.across)

    def pass_y(self, v, k):
        piece = self.half(v, self.py, self.off[k], 0)
        return self.copy(7, piece, piece, v, self.across, k)

    def pass_x(self, v, k):
        piece = self.half(v, self.qy, self.px, 1)
        return self.copy(8, piece, piece, v, self.row(k), k)

    def hand(self, v, role):
        y, k = (self.py, role) if role < self.xs else (self.qy, role - self.xs)
        piece = self.block(v, y, self.off[k])
        return self.copy(9, piece, piece, v, self.mate)

    def handed(self, v):
        kinds = self.phase(v) if self.phases > 1 else slice(None)
        every = self.full.at[kinds, :, :, self.core, :, self.cols(v)]
        return self.copy(9, every, every, v, self.mate)

    def put(self, v, kind, rows):
        p, cols = self.phase(v), self.cols(v)
        shape = (self.ys, self.xs, 2, self.share, self.step)
        self.x[p, kind, :, :, :, :, cols] = rows.astype(BF16).reshape(shape)

    def pair(self, v):
        p, cols = self.phase(v), self.cols(v)
        self.mated(v).wait_recv()
        self.paired[p, :, :, :, :, cols] = (
            self.x[p, :, :, :, self.core, :, cols].astype(F32) + self.mate_in[p, :, :, :, :, cols].astype(F32)
        ).astype(BF16)
        for k in range(1, self.xs):
            self.first_x(v, k).start()
        self.first_y(v).start()

    def cross(self, v):
        p, cols = self.phase(v), self.cols(v)
        for k in range(1, self.xs):
            self.first_x(v, k).wait_recv()
        total = self.paired[p, 0, self.qy, self.px, :, cols].astype(F32)
        for k in range(1, self.xs):
            total = total + self.x1[p, self.off[k], self.qy, :, cols].astype(F32)
        self.sa[p, :, cols] = total.astype(BF16)
        self.second_y(v).start()
        self.first_y(v).wait_recv()
        for k in range(1, self.xs):
            total = self.paired[p, 1, self.py, self.to[k], :, cols].astype(F32) + self.y1[
                p, self.to[k], :, cols
            ].astype(F32)
            self.sb[p, self.to[k], :, cols] = total.astype(BF16)
            self.second_x(v, k).start()

    def totals(self, v):
        p, cols = self.phase(v), self.cols(v)
        self.second_y(v).wait_recv()
        for k in range(1, self.xs):
            self.second_x(v, k).wait_recv()
        one = self.paired[p, 0, self.py, self.px, :, cols].astype(F32) + self.y2[p, :, cols].astype(F32)
        two = self.paired[p, 1, self.py, self.px, :, cols].astype(F32) + self.y1[p, self.px, :, cols].astype(F32)
        for k in range(1, self.xs):
            one = one + self.x1[p, self.off[k], self.py, :, cols].astype(F32)
            two = two + self.x2[p, self.off[k], :, cols].astype(F32)
        return one, two

    def keep(self, v, kind, rows):
        self.full[kind, self.py, self.px, self.core, :, self.cols(v)] = rows.astype(BF16)

    def spread(self, v):
        for k in range(1, self.xs):
            self.gather_x(v, k).start()
        self.gather_y(v).start()
        self.hand(v, 0).start()

    def relay(self, v):
        for k in range(1, self.xs):
            self.gather_x(v, k).wait_recv()
            self.pass_y(v, k).start()
        self.gather_y(v).wait_recv()
        for k in range(1, self.xs):
            self.pass_x(v, k).start()
        for role in range(1, self.xs + 1):
            self.hand(v, role).start()

    def relay_last(self, v):
        for k in range(1, self.xs):
            self.pass_y(v, k).wait_recv()
            self.pass_x(v, k).wait_recv()
            self.hand(v, self.xs + k).start()

    def complete(self, v):
        self.handed(v).wait_recv()

    def rows(self, v, kind):
        cols = self.cols(v)
        return self.full[kind, :, :, :, :, cols].reshape(self.n * self.share, self.step)

    def drain(self):
        full = self.full
        mine, half = full.at[:, self.py, self.px, self.core], full.at[0, self.py, self.px, self.core]
        every = full.at[:, :, :, self.core]
        self.copy(0, self.x.at[:, :, :, :, 1 - self.core], self.mate_in, 0, self.mate).wait_send()
        self.copy(2, self.paired.at[:, 1, self.qy], self.y1, 0, self.across).wait_send()
        self.copy(3, self.sa, self.y2, 0, self.across).wait_send()
        self.copy(6, mine, mine, 0, self.across).wait_send()
        self.copy(9, every, every, 0, self.mate).wait_send()
        for k in range(1, self.xs):
            self.copy(1, self.paired.at[:, 0, :, self.to[k]], self.x1.at[:, self.px], 0, self.row(k), k).wait_send()
            self.copy(4, self.sb.at[:, self.to[k]], self.x2.at[:, self.px], 0, self.row(k), k).wait_send()
            self.copy(5, mine, mine, 0, self.row(k), k).wait_send()
            self.copy(7, half, half, 0, self.across, k).wait_send()
            self.copy(8, half, half, 0, self.row(k), k).wait_send()


LAGS = dict(pair=1, cross=4, unit=4, totals=7, relay=9, last=11, done=12)
LATER = dict(pair=1, cross=4, totals=6, relay=8, last=10, done=11)


def staged(i, lag, steps, body):
    v = i - lag

    @pl.when((v >= 0) & (v < steps))
    def _():
        body(v)


DEEP = 4
SLOTS = 3


def squares(along_ref, before_ref, norms):
    rows, width = along_ref.shape
    step = tile_of(rows, 32)

    def body(i, sums):
        at = pl.ds(pl.multiple_of(i * step, step), step)
        along = along_ref[at, :].astype(F32)
        before = before_ref[at, :].astype(F32)
        products = (along * along, along * before, before * before)
        return tuple(have + folded(product) for have, product in zip(sums, products))

    zero = jnp.zeros((8, width), F32)
    sums = lax.fori_loop(0, rows // step, body, (zero, zero, zero))
    for kind in range(3):
        norms[kind] += lanes(sums[kind])


def early_kernel(n, t, width, *refs):
    (tokens, targets, gate, up, down, along_gate, along_up, along_down, before_gate, before_up, before_down) = refs[:11]
    (out_tokens, out_units, out_keeps, out_grads, out_before, norms) = refs[11:17]
    (tok, keeps, bx, weights, downs, alongs, wide, tall, acc, zx, zin, gz) = refs[17:29]
    (tok_s, tok_r, w_sem, d_sem, wide_sem, tall_sem, zs, zr, gs, gr, o_sem) = refs[29:40]
    width.bind(refs[40:])
    chunks, steps, step = width.chunks, width.steps, width.step
    share, depth = tokens.shape
    rows = t * share
    me = lax.axis_index("tp")
    spots = [lax.rem(me + s, t) for s in range(1, t)]
    sources = [lax.rem(me + t - s, t) for s in range(1, t)]

    def col(v):
        return width.cols(v)

    def load(v, one, two, start):
        slot = lax.rem(v, DEEP)
        for kind, ref in enumerate((one, two)):
            copy = pltpu.make_async_copy(ref.at[:, col(v)], weights.at[slot, kind], w_sem.at[slot, kind])
            if start:
                copy.start()
            else:
                copy.wait()

    def fetch(v):
        @pl.when(v < chunks)
        def _():
            load(v, gate, up, True)

        @pl.when((v >= chunks) & (v < steps))
        def _():
            load(v, along_gate, along_up, True)

    for v in range(DEEP):
        fetch(jnp.int32(v))

    def wide_copies(one, two, c):
        slot = lax.rem(c, SLOTS)
        return [
            pltpu.make_async_copy(ref.at[:, col(c)], wide.at[slot, kind], wide_sem.at[slot, kind])
            for kind, ref in enumerate((one, two))
            if ref is not None
        ]

    def tall_copies(c):
        slot = lax.rem(c, SLOTS)
        return [
            pltpu.make_async_copy(ref.at[col(c), :], tall.at[slot, kind], tall_sem.at[slot, kind])
            for kind, ref in enumerate((along_down, before_down))
        ]

    def open_stream(copies):
        for c in range(min(SLOTS, chunks)):
            for copy in copies(jnp.int32(c)):
                copy.start()

    def turn(copies, c, body):
        for copy in copies(c):
            copy.wait()
        body(c, lax.rem(c, SLOTS))

        @pl.when(c + SLOTS < chunks)
        def _():
            for copy in copies(c + SLOTS):
                copy.start()

    def run_stream(copies, body):
        @pl.loop(0, chunks)
        def _(c):
            turn(copies, c, body)

    gate_stream = functools.partial(wide_copies, along_gate, before_gate)
    up_stream = functools.partial(wide_copies, along_up, before_up)
    again_stream = functools.partial(wide_copies, None, before_gate)
    open_stream(gate_stream)
    load_down = pltpu.make_async_copy(down, downs, d_sem.at[0])
    load_along = pltpu.make_async_copy(along_down, alongs, d_sem.at[1])

    norms[...] = jnp.zeros_like(norms)
    greet(width.partners() + [{"tp": spot} for spot in spots])

    def gather(i):
        return remote(tokens, tok.at[me], tok_s.at[i], tok_r.at[i], {"tp": spots[i]})

    for i in range(t - 1):
        gather(i).start()
    tok[me] = tokens[...]

    def norm_wide(c, slot):
        squares(wide.at[slot, 0], wide.at[slot, 1], norms)

    run_stream(gate_stream, norm_wide)
    open_stream(up_stream)
    for i in range(t - 1):
        gather(i).wait_recv()

    def everyone():
        return tok[...].reshape(rows, depth)

    acc[...] = jnp.zeros_like(acc)

    def front(v):
        load(v, gate, up, False)
        slot = lax.rem(v, DEEP)
        for kind in range(2):
            width.put(v, kind, dot(everyone(), weights[slot, kind]))
        width.mated(v).start()
        fetch(v + DEEP)

    def sums(v):
        one, two = width.totals(v)
        cols = col(v)
        p = width.phase(v)

        @pl.when(p == 0)
        def _():
            keeps[0, :, cols] = one
            keeps[1, :, cols] = two
            width.keep(v, 0, one * jax.nn.sigmoid(one) * two)

        @pl.when(p == 1)
        def _():
            keeps[2, :, cols] = one
            keeps[3, :, cols] = two
            gate_sum, up_sum = keeps[0, :, cols], keeps[1, :, cols]
            logistic = jax.nn.sigmoid(gate_sum)
            slope = logistic * (1.0 + gate_sum * (1.0 - logistic))
            width.keep(v, 1, slope * up_sum * one + gate_sum * logistic * two)

        width.spread(v)

    def middle(v):
        width.complete(v)
        p, at = width.phase(v), col(v)

        @pl.when(v == 0)
        def _():
            load_down.wait()

        @pl.when(v == chunks)
        def _():
            load_along.wait()

        @pl.when(p == 0)
        def _():
            acc[0] += dot(width.rows(v, 0), downs[at, :])

        @pl.when(p == 1)
        def _():
            acc[1] += dot(width.rows(v, 1), downs[at, :]) + dot(width.rows(v, 0), alongs[at, :])

    def z_first(p, i):
        return remote(zx.at[p, spots[i]], zin.at[p, me], zs.at[p, i], zr.at[p, i], {"tp": spots[i]})

    def z_second(p, i):
        return remote(gz.at[p, me], gz.at[p, me], gs.at[p, i], gr.at[p, i], {"tp": spots[i]})

    def z_send(p):
        zx[p] = acc[p].astype(BF16).reshape(t, share, depth)
        for i in range(t - 1):
            z_first(p, i).start()

    def z_finish(p):
        for i in range(t - 1):
            z_first(p, i).wait_recv()
        total = zx[p, me].astype(F32)
        for at in sources:
            total = total + zin[p, at].astype(F32)
        if p == 0:
            total = total - targets[...].astype(F32)
        gz[p, me] = (total / rows).astype(BF16)
        for i in range(t - 1):
            z_second(p, i).start()

    def before_of(kind):
        def body(c, slot):
            bx[kind, :, col(c)] = dot(everyone(), wide[slot, 1]).astype(BF16)

        return body

    def norm_and_before(c, slot):
        norm_wide(c, slot)
        before_of(1)(c, slot)

    def norm_tall(c, slot):
        squares(tall.at[slot, 0], tall.at[slot, 1], norms)

    def unit(v):
        @pl.when(v < chunks)
        def _():
            turn(up_stream, v, norm_and_before)

        @pl.when(v >= chunks)
        def _():
            turn(tall_copies, v - chunks, norm_tall)

    ready = chunks - 1 + LAGS["done"]
    last = steps + LAGS["done"]
    settle = min(ready + 4, last - 1)

    @pl.loop(0, last)
    def _(i):
        staged(i, 0, steps, front)
        staged(i, LAGS["unit"], steps, unit)
        staged(i, LAGS["cross"], steps, width.cross)
        staged(i, LAGS["totals"], steps, sums)
        staged(i, LAGS["relay"], steps, width.relay)
        staged(i, LAGS["last"], steps, width.relay_last)
        staged(i, LAGS["done"], steps, middle)
        staged(i, LAGS["pair"], steps, width.pair)

        @pl.when(i == min(4, ready))
        def _():
            load_down.start()

        @pl.when(i == min(7, ready))
        def _():
            open_stream(tall_copies)

        @pl.when(i == min(11, ready))
        def _():
            load_along.start()

        @pl.when(i == ready)
        def _():
            z_send(0)

        @pl.when(i == settle)
        def _():
            z_finish(0)

    z_send(1)
    open_stream(again_stream)

    stores = [
        pltpu.make_async_copy(tok, out_tokens, o_sem.at[0]),
        pltpu.make_async_copy(width.full, out_units, o_sem.at[1]),
        pltpu.make_async_copy(keeps, out_keeps, o_sem.at[2]),
    ]
    for store in stores:
        store.start()
    run_stream(again_stream, before_of(0))
    stores.append(pltpu.make_async_copy(bx, out_before, o_sem.at[3]))
    stores[-1].start()
    z_finish(1)

    for p in range(2):
        for i in range(t - 1):
            z_second(p, i).wait_recv()
    stores.append(pltpu.make_async_copy(gz, out_grads, o_sem.at[4]))
    stores[-1].start()
    for i in range(t - 1):
        gather(i).wait_send()
        for p in range(2):
            z_first(p, i).wait_send()
            z_second(p, i).wait_send()
    width.drain()
    for store in stores:
        store.wait()


def early(n, t, tokens, targets, gate, up, down, along_gate, along_up, along_down, before_gate, before_up, before_down):
    share, depth = tokens.shape
    width = gate.shape[1]
    rows = t * share
    chunks = width // tile_of(width, max(128, width // 8))
    plan = Width(n, 2, chunks, 2, rows // n, width)
    step = plan.step
    keeps = (4, plan.share, width)
    units = (2, plan.ys, plan.xs, 2, plan.share, width)
    z = (2, t, share, depth)
    return pl.pallas_call(
        functools.partial(early_kernel, n, t, plan),
        out_shape=[
            jax.ShapeDtypeStruct((t, share, depth), BF16),
            jax.ShapeDtypeStruct(units, BF16),
            jax.ShapeDtypeStruct(keeps, F32),
            jax.ShapeDtypeStruct(z, BF16),
            jax.ShapeDtypeStruct((2, rows, width), BF16),
            jax.ShapeDtypeStruct((3, 8, 128), F32),
        ],
        in_specs=[WHOLE, WHOLE] + [ANY] * 9,
        out_specs=[ANY] * 5 + [WHOLE],
        scratch_shapes=[
            VMEM((t, share, depth), BF16),
            VMEM(keeps, F32),
            VMEM((2, rows, width), BF16),
            VMEM((DEEP, 2, depth, step), BF16),
            VMEM((width, depth), BF16),
            VMEM((width, depth), BF16),
            VMEM((SLOTS, 2, depth, step), BF16),
            VMEM((SLOTS, 2, step, depth), BF16),
            VMEM((2, rows, depth), F32),
            VMEM(z, BF16),
            VMEM(z, BF16),
            VMEM(z, BF16),
            DMA((t - 1,)),
            DMA((t - 1,)),
            DMA((DEEP, 2)),
            DMA((2,)),
            DMA((SLOTS, 2)),
            DMA((SLOTS, 2)),
            DMA((2, t - 1)),
            DMA((2, t - 1)),
            DMA((2, t - 1)),
            DMA((2, t - 1)),
            DMA((5,)),
        ]
        + plan.scratch(),
        compiler_params=pltpu.CompilerParams(collective_id=1, has_side_effects=True, vmem_limit_bytes=LIMIT),
    )(tokens, targets, gate, up, down, along_gate, along_up, along_down, before_gate, before_up, before_down)


def late_kernel(n, t, entries, width, *refs):
    (tokens, units, keeps_in, grads_in, before_in, norms, down, along, before) = refs[:9]
    wide_in, beta_prev, out_dirs, scales, alongs, wide_out = refs[9:12], refs[12], refs[13], refs[14], refs[18], refs[19:22]
    tall, hidden, grads = refs[15:18]
    (keeps, bx, downs, befores, sums, gram, swap_gram, dp_in, total_dp, tp_in) = refs[22:32]
    (in_sem, m_sem, w_sem, s1, r1, s2, r2) = refs[32:39]
    width.bind(refs[39:])
    chunks, steps, step = width.chunks, width.steps, width.step
    depth = down.shape[1]
    rows = n * width.share
    dp, tp = lax.axis_index("dp"), lax.axis_index("tp")
    dp_spots = [lax.rem(dp + s, n) for s in range(1, n)]
    tp_spots = [lax.rem(tp + s, t) for s in range(1, t)]

    loads = [
        pltpu.make_async_copy(src, dst, in_sem.at[i])
        for i, (src, dst) in enumerate(((grads_in, grads), (units, hidden), (keeps_in, keeps), (before_in, bx)))
    ]

    def matrix(which, c):
        at, slot = width.cols(c), lax.rem(c, DEEP)
        src = (down, along, before)[which].at[at, :]
        dst = alongs.at[at, :] if which == 1 else (downs, befores)[which // 2].at[slot]
        return pltpu.make_async_copy(src, dst, m_sem.at[which, slot])

    def fetch(c):
        @pl.when(c < steps)
        def _():
            for which in range(3):
                matrix(which, c).start()

    def ahead(c):
        for src, dst, sem in zip(wide_in, wide_out, range(3)):
            at = width.cols(c)
            pltpu.make_async_copy(src.at[:, at], dst.at[:, at], w_sem.at[sem]).start()

    for load in loads:
        load.start()
    for c in range(2):
        fetch(jnp.int32(c))
    sums[...] = jnp.zeros_like(sums)
    gram[...] = jnp.zeros_like(gram)
    swap_gram[...] = jnp.zeros_like(swap_gram)
    tall[...] = tokens[...].reshape(rows, depth).T
    greet([{"dp": spot} for spot in dp_spots] + [{"tp": spot} for spot in tp_spots])
    loads[0].wait()
    for c in range(2, DEEP - 1):
        fetch(jnp.int32(c))
    for load in loads[1:]:
        load.wait()

    def both():
        return grads[...].reshape(2 * rows, depth)

    def unit(v, kind):
        return hidden[kind, :, :, :, :, width.cols(v)].reshape(rows, step)

    def crossed(which, v, products):
        value = products[:rows] * unit(v, 1).astype(F32) + products[rows:] * unit(v, 0).astype(F32)
        sums[which] += lanes(folded(value))

    def back(v):
        matrix(0, v).wait()
        matrix(1, v).wait()
        at = width.cols(v)
        weighted = against(both(), downs[lax.rem(v, DEEP)])
        moved = against(both(), alongs[at, :])
        width.put(v, 0, weighted[:rows])
        width.put(v, 1, weighted[rows:] + moved[:rows])
        width.mated(v).start()
        crossed(1, v, moved)
        fetch(v + DEEP - 1)

    def extra(v):
        matrix(2, v).wait()
        crossed(2, v, against(both(), befores[lax.rem(v, DEEP)]))
        swapped = jnp.concatenate([unit(v, 1), unit(v, 0)])
        swap_gram[...] += against(swapped, swapped)

    def middle(v):
        grad_hidden, grad_hidden_dir = width.totals(v)
        cols = width.cols(v)
        gate_sum, up_sum, gate_dir, up_dir = (keeps[k, :, cols] for k in range(4))
        logistic = jax.nn.sigmoid(gate_sum)
        activation = gate_sum * logistic
        slope = logistic * (1.0 + gate_sum * (1.0 - logistic))
        curve = logistic * (1.0 - logistic) * (2.0 + gate_sum * (1.0 - 2.0 * logistic))
        grad_gate = (
            grad_hidden_dir * up_sum * slope + grad_hidden * up_dir * slope + grad_hidden * up_sum * curve * gate_dir
        ).astype(BF16)
        grad_up = (grad_hidden_dir * activation + grad_hidden * slope * gate_dir).astype(BF16)
        width.keep(v, 0, grad_gate)
        width.keep(v, 1, grad_up)
        width.spread(v)
        sums[1] += lanes(folded(grad_gate.astype(F32) * gate_dir + grad_up.astype(F32) * up_dir))

    def finish(v):
        width.complete(v)
        cols = width.cols(v)
        for kind in range(2):
            part = width.rows(v, kind)
            out_dirs[kind, :, cols] = part
            gram[...] += against(part, part)
            sums[2] += lanes(folded(part.astype(F32) * bx[kind, :, cols].astype(F32)))

    @pl.loop(0, steps + LATER["done"])
    def _(i):
        staged(i, 1, steps, extra)
        staged(i, 0, steps, back)
        staged(i, LATER["cross"], steps, width.cross)
        staged(i, LATER["totals"], steps, middle)
        staged(i, LATER["relay"], steps, width.relay)
        staged(i, LATER["last"], steps, width.relay_last)
        staged(i, LATER["done"], steps, finish)
        staged(i, LATER["pair"], steps, width.pair)
        staged(i, 6, steps, ahead)

    every = tokens[...].reshape(rows, depth)
    sums[0] += lanes(folded(against(every, every) * gram[...])) + lanes(
        folded(against(both(), both()) * swap_gram[...])
    )
    shape = (1, 128)
    own = [jnp.full(shape, jnp.sum(sums[k])) for k in range(3)] + [jnp.full(shape, jnp.sum(norms[k])) for k in range(3)]
    for k in range(6):
        total_dp[k : k + 1] = own[k]
    total_dp[6:8] = jnp.zeros((2, 128), F32)
    dp_in[dp] = total_dp[...]

    first = [
        remote(total_dp, dp_in.at[dp], s1.at[i], r1.at[i], {"dp": spot}) for i, spot in enumerate(dp_spots)
    ]
    for copy in first:
        copy.start()
    for copy in first:
        copy.wait_recv()
    total = dp_in[0]
    for at in range(1, n):
        total = total + dp_in[at]
    tp_in[tp] = total
    second = [
        remote(tp_in.at[tp], tp_in.at[tp], s2.at[i], r2.at[i], {"tp": spot}) for i, spot in enumerate(tp_spots)
    ]
    for copy in second:
        copy.start()
    for copy in second:
        copy.wait_recv()
    total = tp_in[0]
    for at in range(1, t):
        total = total + tp_in[at]
    image_image, image_along, image_before = total[0:1], total[1:2], total[2:3]
    along_along, along_before, before_before = total[3:4], total[4:5], total[5:6]
    beta_old = beta_prev[0]
    alpha_coef = image_along / entries
    square = (
        image_image
        - 2.0 * alpha_coef * image_along
        - 2.0 * beta_old * image_before
        + alpha_coef * alpha_coef * along_along
        + 2.0 * alpha_coef * beta_old * along_before
        + beta_old * beta_old * before_before
    )
    beta_coef = jnp.sqrt(square / entries + 1e-06)
    inverse = 1.0 / beta_coef
    scales[0:1] = alpha_coef
    scales[1:2] = beta_coef
    scales[2:3] = inverse
    scales[3:4] = alpha_coef * inverse
    scales[4:5] = beta_old * inverse
    scales[5:8] = jnp.zeros((3, 128), F32)
    for copy in first + second:
        copy.wait_send()
    width.drain()
    for src, dst, sem in zip(wide_in, wide_out, range(3)):
        pltpu.make_async_copy(src, dst, w_sem.at[sem]).wait()


def late(n, t, entries, tokens, units, keeps, grads, bx, norms, down, along, before, wides, beta_prev):
    width, depth = down.shape
    rows = bx.shape[1]
    chunks = width // tile_of(width, max(128, width // 8))
    plan = Width(n, 1, chunks, 2, rows // n, width)
    small = (8, 128)
    return pl.pallas_call(
        functools.partial(late_kernel, n, t, entries, plan),
        out_shape=[VMEM(bx.shape, BF16), jax.ShapeDtypeStruct(small, F32), VMEM((depth, rows), BF16)]
        + [VMEM(like.shape, BF16) for like in (units, grads, along) + wides],
        in_specs=[WHOLE] + [ANY] * 4 + [WHOLE] + [ANY] * 6 + [pl.BlockSpec(memory_space=pltpu.SMEM)],
        out_specs=[WHOLE] * 9,
        scratch_shapes=[
            VMEM(keeps.shape, F32),
            VMEM(bx.shape, BF16),
            VMEM((DEEP, plan.step, depth), BF16),
            VMEM((DEEP, plan.step, depth), BF16),
            VMEM((3,) + small, F32),
            VMEM((rows, rows), F32),
            VMEM((2 * rows, 2 * rows), F32),
            VMEM((n,) + small, F32),
            VMEM(small, F32),
            VMEM((t,) + small, F32),
            DMA((4,)),
            DMA((3, DEEP)),
            DMA((3,)),
            DMA((n - 1,)),
            DMA((n - 1,)),
            DMA((t - 1,)),
            DMA((t - 1,)),
        ]
        + plan.scratch(),
        compiler_params=pltpu.CompilerParams(collective_id=2, has_side_effects=True, vmem_limit_bytes=LATE),
    )(tokens, units, keeps, grads, bx, norms, down, along, before, *wides, beta_prev)


def next_kernel(scales, before_up, before_down, dirs, tall, units, grads, along_down, along_gate, along_up, before_gate, *refs):
    out_gate, out_up, out_down, coefs, slopes, ups, downs, wides, talls, b_sem, o_sem = refs
    inverse, alpha, beta = scales[2, 0], scales[3, 0], scales[4, 0]
    depth, width = along_gate.shape
    rows = dirs.shape[1]
    tile, part, deep = wides.shape[2], tile_of(depth, 256), downs.shape[0]
    count = width // tile

    def piece(j):
        return pl.ds(pl.multiple_of(j * tile, tile), tile)

    def previous(which, j):
        if which == 0:
            return pltpu.make_async_copy(before_up.at[:, piece(j)], ups.at[:, piece(j)], b_sem.at[0, j])
        slot = lax.rem(j, deep)
        return pltpu.make_async_copy(before_down.at[piece(j), :], downs.at[slot], b_sem.at[1, slot])

    for j in range(count):
        previous(0, jnp.int32(j)).start()
    coefs[0] = scales[0, 0]
    coefs[1] = scales[1, 0]

    def scaled(values):
        return (values.astype(F32) * inverse).astype(BF16)

    def blend(image, along, before):
        return (image - along.astype(F32) * alpha - before.astype(F32) * beta).astype(BF16)

    def store(which, j):
        slot = lax.rem(j, DEEP)
        if which < 2:
            dst, src = (out_gate, out_up)[which].at[:, piece(j)], wides.at[slot]
        else:
            dst, src = out_down.at[piece(j), :], talls.at[slot]
        return pltpu.make_async_copy(src, dst, o_sem.at[which // 2, slot])

    for which, (along, before) in enumerate(((along_gate, before_gate), (along_up, ups))):
        @pl.loop(0, count)
        def _(j):
            slot, cols = lax.rem(j, DEEP), piece(j)
            if which == 0:
                @pl.when(j >= DEEP)
                def _():
                    store(0, j).wait()

                @pl.when(j == count // 2)
                def _():
                    for at in range(min(deep, count)):
                        previous(1, jnp.int32(at)).start()
            else:
                previous(0, j).wait()
                store(0, j).wait()
            way = scaled(dirs[which, :, cols])
            for at in range(0, depth, part):
                here = slice(at, at + part)
                wides[slot, here, :] = blend(dot(tall[here, :], way), along[here, cols], before[here, cols])
            store(which, j).start()

    slopes[...] = scaled(grads[...].reshape(2 * rows, depth))

    @pl.loop(0, count)
    def _(j):
        slot, cols = lax.rem(j, DEEP), piece(j)
        place = lax.rem(j, deep)

        @pl.when(j >= DEEP)
        def _():
            store(2, j).wait()

        previous(1, j).wait()
        swapped = jnp.concatenate([units[k, :, :, :, :, cols].reshape(rows, tile) for k in (1, 0)]).T
        for at in range(0, depth, part):
            here = slice(at, at + part)
            talls[slot, :, here] = blend(dot(swapped, slopes[:, here]), along_down[cols, here], downs[place, :, here])
        store(2, j).start()

        @pl.when(j + deep < count)
        def _():
            previous(1, j + deep).start()

    for j in range(min(DEEP, count)):
        store(0, jnp.int32(j)).wait()
        store(2, jnp.int32(j)).wait()


def next_parts(scales, before_up, before_down, *held):
    depth, width = before_up.shape
    rows = held[0].shape[1]
    tile = tile_of(width, max(128, min(256, width // DEEP)))
    smem = pl.BlockSpec(memory_space=pltpu.SMEM)
    count = width // tile
    deep = min(2 * DEEP, count)
    return pl.pallas_call(
        next_kernel,
        out_shape=[jax.ShapeDtypeStruct((depth, width), BF16)] * 2
        + [jax.ShapeDtypeStruct((width, depth), BF16), jax.ShapeDtypeStruct((2,), F32)],
        in_specs=[smem] + [ANY] * 2 + [WHOLE] * len(held),
        out_specs=[ANY] * 3 + [smem],
        scratch_shapes=[
            VMEM((2 * rows, depth), BF16),
            VMEM((depth, width), BF16),
            VMEM((deep, tile, depth), BF16),
            VMEM((DEEP, depth, tile), BF16),
            VMEM((DEEP, tile, depth), BF16),
            DMA((2, count)),
            DMA((2, DEEP)),
        ],
        compiler_params=pltpu.CompilerParams(vmem_limit_bytes=LAST),
    )(scales, before_up, before_down, *held)


def on_device(
    n,
    t,
    tokens,
    targets,
    gate_weight,
    up_weight,
    down_weight,
    direction_gate,
    direction_up,
    direction_down,
    previous_gate,
    previous_up,
    previous_down,
    beta_prev,
):
    everyone, units, keeps, grads, bx, norms = early(
        n,
        t,
        tokens,
        targets,
        gate_weight,
        up_weight,
        down_weight,
        direction_gate,
        direction_up,
        direction_down,
        previous_gate,
        previous_up,
        previous_down,
    )
    entries = float(n * t * (gate_weight.size + up_weight.size + down_weight.size))
    wides = (direction_gate, direction_up, previous_gate)
    dirs, scales, *held = late(
        n, t, entries, everyone, units, keeps, grads, bx, norms, down_weight, direction_down, previous_down, wides, beta_prev
    )
    held = [pltpu.with_memory_space_constraint(array, VMEM) for array in [dirs] + held]
    return tuple(next_parts(scales, previous_up, previous_down, *held))


def solution(mesh):
    wide, tall = P("dp", "tp"), P("tp", "dp")
    in_specs = (tall, tall, wide, wide, tall, wide, wide, tall, wide, wide, tall, P())
    return jax.shard_map(
        functools.partial(on_device, mesh.shape["dp"], mesh.shape["tp"]),
        mesh=mesh,
        in_specs=in_specs,
        out_specs=(wide, wide, tall, P()),
        check_vma=False,
    )
```

```python
import functools

import jax
import jax.numpy as jnp
from jax import lax
from jax.experimental import pallas as pl
from jax.experimental.pallas import tpu as pltpu
from jax.sharding import PartitionSpec as P

MESH = pl.DeviceIdType.MESH
VMEM = pltpu.VMEM
DMA = pltpu.SemaphoreType.DMA
ANY = pl.BlockSpec(memory_space=pl.ANY)
WHOLE = pl.BlockSpec(memory_space=pltpu.VMEM)
F32 = jnp.float32
BF16 = jnp.bfloat16
LIMIT = 62 * 1024 * 1024
LATE = 22 * 1024 * 1024
LAST = LATE


def tile_of(size, most):
    tile = min(size, most)
    while size % tile:
        tile //= 2
    return tile


def dot(one, two):
    return jnp.dot(one, two, preferred_element_type=F32)


def against(one, two):
    return lax.dot_general(one, two, (((1,), (1,)), ((), ())), preferred_element_type=F32)


def greet(targets):
    barrier = pltpu.get_barrier_semaphore()
    for target in targets:
        pl.semaphore_signal(barrier, inc=1, device_id=target, device_id_type=MESH)
    pl.semaphore_wait(barrier, len(targets))


def remote(src, dst, send_sem, recv_sem, target):
    return pltpu.make_async_remote_copy(
        src_ref=src, dst_ref=dst, send_sem=send_sem, recv_sem=recv_sem, device_id=target, device_id_type=MESH
    )


def folded(values, width=None):
    rows, cols = values.shape
    return values.reshape(rows // 8, 8, cols).sum(axis=0)


def lanes(values):
    total = values[:, :128]
    for at in range(128, values.shape[1], 128):
        total = total + values[:, at : at + 128]
    return total


class Width:
    def __init__(self, n, phases, chunks, kinds, share, width):
        self.n, self.phases, self.chunks, self.kinds = n, phases, chunks, kinds
        self.share, self.width = share, width
        self.steps = phases * chunks
        self.ys, self.xs = 2, n // 4
        self.step = width // chunks
        self.slots = min(self.steps, 8)

    def scratch(self):
        p, y, x, share, width, v = self.phases, self.ys, self.xs, self.share, self.width, self.steps
        return [
            VMEM((p, 2, y, x, 2, share, width), BF16),
            VMEM((p, 2, y, x, share, width), BF16),
            VMEM((p, 2, y, x, share, width), BF16),
            VMEM((p, x, y, share, width), BF16),
            VMEM((p, x, share, width), BF16),
            VMEM((p, share, width), BF16),
            VMEM((p, x, share, width), BF16),
            VMEM((p, share, width), BF16),
            VMEM((p, x, share, width), BF16),
            VMEM((self.kinds, y, x, 2, share, width), BF16),
        ] + [
            DMA(shape)
            for one, slots in zip((1, x - 1, 1, 1, x - 1, x - 1, 1, x - 1, x - 1, 1), [self.slots] * 9 + [v])
            for shape in ((one,), (slots, one))
        ]

    def bind(self, refs):
        (self.x, self.mate_in, self.paired, self.x1, self.y1, self.y2, self.x2, self.sa, self.sb, self.full) = refs[:10]
        sems = refs[10:]
        self.sems = [(sems[i], sems[i + 1]) for i in range(0, len(sems), 2)]
        me = lax.axis_index("dp")
        self.core = lax.rem(me, 2)
        chip = lax.div(me, 2)
        self.px, self.py = lax.rem(chip, self.xs), lax.div(chip, self.xs)
        self.qy = 1 - self.py
        self.mate = self.at(self.py, self.px, 1 - self.core)
        self.across = self.at(self.qy, self.px, self.core)
        self.to = [lax.rem(self.px + s, self.xs) for s in range(self.xs)]
        self.off = [lax.rem(self.px + self.xs - s, self.xs) for s in range(self.xs)]

    def at(self, y, x, core):
        return {"dp": (y * self.xs + x) * 2 + core}

    def partners(self):
        row = [self.at(self.py, self.to[s], self.core) for s in range(1, self.xs)]
        return [self.mate, self.across] + row

    def cols(self, v, part=0, parts=1):
        size = self.step // parts
        start = lax.rem(v, self.chunks) * self.step + part * size
        return pl.ds(pl.multiple_of(start, size), size)

    def phase(self, v):
        return lax.div(v, self.chunks)

    def row(self, s):
        return self.at(self.py, self.to[s], self.core)

    def copy(self, which, src, dst, v, target, k=1):
        send, recv = self.sems[which]
        return remote(src, dst, send.at[k - 1], recv.at[lax.rem(v, recv.shape[0]), k - 1], target)

    def mated(self, v):
        p, cols = self.phase(v), self.cols(v)
        src = self.x.at[p, :, :, :, 1 - self.core, :, cols]
        return self.copy(0, src, self.mate_in.at[p, :, :, :, :, cols], v, self.mate)

    def first_x(self, v, k):
        p, cols = self.phase(v), self.cols(v)
        src = self.paired.at[p, 0, :, self.to[k], :, cols]
        return self.copy(1, src, self.x1.at[p, self.px, :, :, cols], v, self.row(k), k)

    def first_y(self, v):
        p, cols = self.phase(v), self.cols(v)
        return self.copy(2, self.paired.at[p, 1, self.qy, :, :, cols], self.y1.at[p, :, :, cols], v, self.across)

    def second_y(self, v):
        p, cols = self.phase(v), self.cols(v)
        return self.copy(3, self.sa.at[p, :, cols], self.y2.at[p, :, cols], v, self.across)

    def second_x(self, v, k):
        p, cols = self.phase(v), self.cols(v)
        return self.copy(4, self.sb.at[p, self.to[k], :, cols], self.x2.at[p, self.px, :, cols], v, self.row(k), k)

    def block(self, v, y, x):
        if self.phases > 1:
            return self.full.at[self.phase(v), y, x, self.core, :, self.cols(v)]
        return self.full.at[:, y, x, self.core, :, self.cols(v)]

    def half(self, v, y, x, part):
        if self.phases == 1:
            return self.full.at[part, y, x, self.core, :, self.cols(v)]
        if self.step % 256 == 0:
            return self.full.at[self.phase(v), y, x, self.core, :, self.cols(v, part, 2)]
        rows = pl.ds(part * (self.share // 2), self.share // 2)
        return self.full.at[self.phase(v), y, x, self.core, rows, self.cols(v)]

    def gather_x(self, v, k):
        mine = self.block(v, self.py, self.px)
        return self.copy(5, mine, mine, v, self.row(k), k)

    def gather_y(self, v):
        mine = self.block(v, self.py, self.px)
        return self.copy(6, mine, mine, v, self.across)

    def pass_y(self, v, k):
        piece = self.half(v, self.py, self.off[k], 0)
        return self.copy(7, piece, piece, v, self.across, k)

    def pass_x(self, v, k):
        piece = self.half(v, self.qy, self.px, 1)
        return self.copy(8, piece, piece, v, self.row(k), k)

    def hand(self, v, role):
        y, k = (self.py, role) if role < self.xs else (self.qy, role - self.xs)
        piece = self.block(v, y, self.off[k])
        return self.copy(9, piece, piece, v, self.mate)

    def handed(self, v):
        kinds = self.phase(v) if self.phases > 1 else slice(None)
        every = self.full.at[kinds, :, :, self.core, :, self.cols(v)]
        return self.copy(9, every, every, v, self.mate)

    def put(self, v, kind, rows):
        p, cols = self.phase(v), self.cols(v)
        shape = (self.ys, self.xs, 2, self.share, self.step)
        self.x[p, kind, :, :, :, :, cols] = rows.astype(BF16).reshape(shape)

    def pair(self, v):
        p, cols = self.phase(v), self.cols(v)
        self.mated(v).wait_recv()
        self.paired[p, :, :, :, :, cols] = (
            self.x[p, :, :, :, self.core, :, cols].astype(F32) + self.mate_in[p, :, :, :, :, cols].astype(F32)
        ).astype(BF16)
        for k in range(1, self.xs):
            self.first_x(v, k).start()
        self.first_y(v).start()

    def cross(self, v):
        p, cols = self.phase(v), self.cols(v)
        for k in range(1, self.xs):
            self.first_x(v, k).wait_recv()
        total = self.paired[p, 0, self.qy, self.px, :, cols].astype(F32)
        for k in range(1, self.xs):
            total = total + self.x1[p, self.off[k], self.qy, :, cols].astype(F32)
        self.sa[p, :, cols] = total.astype(BF16)
        self.second_y(v).start()
        self.first_y(v).wait_recv()
        for k in range(1, self.xs):
            total = self.paired[p, 1, self.py, self.to[k], :, cols].astype(F32) + self.y1[
                p, self.to[k], :, cols
            ].astype(F32)
            self.sb[p, self.to[k], :, cols] = total.astype(BF16)
            self.second_x(v, k).start()

    def totals(self, v):
        p, cols = self.phase(v), self.cols(v)
        self.second_y(v).wait_recv()
        for k in range(1, self.xs):
            self.second_x(v, k).wait_recv()
        one = self.paired[p, 0, self.py, self.px, :, cols].astype(F32) + self.y2[p, :, cols].astype(F32)
        two = self.paired[p, 1, self.py, self.px, :, cols].astype(F32) + self.y1[p, self.px, :, cols].astype(F32)
        for k in range(1, self.xs):
            one = one + self.x1[p, self.off[k], self.py, :, cols].astype(F32)
            two = two + self.x2[p, self.off[k], :, cols].astype(F32)
        return one, two

    def keep(self, v, kind, rows):
        self.full[kind, self.py, self.px, self.core, :, self.cols(v)] = rows.astype(BF16)

    def spread(self, v):
        for k in range(1, self.xs):
            self.gather_x(v, k).start()
        self.gather_y(v).start()
        self.hand(v, 0).start()

    def relay(self, v):
        for k in range(1, self.xs):
            self.gather_x(v, k).wait_recv()
            self.pass_y(v, k).start()
        self.gather_y(v).wait_recv()
        for k in range(1, self.xs):
            self.pass_x(v, k).start()
        for role in range(1, self.xs + 1):
            self.hand(v, role).start()

    def relay_last(self, v):
        for k in range(1, self.xs):
            self.pass_y(v, k).wait_recv()
            self.pass_x(v, k).wait_recv()
            self.hand(v, self.xs + k).start()

    def complete(self, v):
        self.handed(v).wait_recv()

    def rows(self, v, kind):
        cols = self.cols(v)
        return self.full[kind, :, :, :, :, cols].reshape(self.n * self.share, self.step)

    def drain(self):
        full = self.full
        mine, half = full.at[:, self.py, self.px, self.core], full.at[0, self.py, self.px, self.core]
        every = full.at[:, :, :, self.core]
        self.copy(0, self.x.at[:, :, :, :, 1 - self.core], self.mate_in, 0, self.mate).wait_send()
        self.copy(2, self.paired.at[:, 1, self.qy], self.y1, 0, self.across).wait_send()
        self.copy(3, self.sa, self.y2, 0, self.across).wait_send()
        self.copy(6, mine, mine, 0, self.across).wait_send()
        self.copy(9, every, every, 0, self.mate).wait_send()
        for k in range(1, self.xs):
            self.copy(1, self.paired.at[:, 0, :, self.to[k]], self.x1.at[:, self.px], 0, self.row(k), k).wait_send()
            self.copy(4, self.sb.at[:, self.to[k]], self.x2.at[:, self.px], 0, self.row(k), k).wait_send()
            self.copy(5, mine, mine, 0, self.row(k), k).wait_send()
            self.copy(7, half, half, 0, self.across, k).wait_send()
            self.copy(8, half, half, 0, self.row(k), k).wait_send()


LAGS = dict(pair=1, cross=4, unit=4, totals=7, relay=9, last=11, done=12)
LATER = dict(pair=1, cross=4, totals=6, relay=8, last=10, done=11)


def staged(i, lag, steps, body):
    v = i - lag

    @pl.when((v >= 0) & (v < steps))
    def _():
        body(v)


DEEP = 4
SLOTS = 3


def squares(along_ref, before_ref, norms):
    rows, width = along_ref.shape
    step = tile_of(rows, 32)

    def body(i, sums):
        at = pl.ds(pl.multiple_of(i * step, step), step)
        along = along_ref[at, :].astype(F32)
        before = before_ref[at, :].astype(F32)
        products = (along * along, along * before, before * before)
        return tuple(have + folded(product) for have, product in zip(sums, products))

    zero = jnp.zeros((8, width), F32)
    sums = lax.fori_loop(0, rows // step, body, (zero, zero, zero))
    for kind in range(3):
        norms[kind] += lanes(sums[kind])


def early_kernel(n, t, width, *refs):
    (tokens, targets, gate, up, down, along_gate, along_up, along_down, before_gate, before_up, before_down) = refs[:11]
    (out_tokens, out_units, out_keeps, out_grads, out_before, norms) = refs[11:17]
    (tok, keeps, bx, weights, downs, alongs, wide, tall, acc, zx, zin, gz) = refs[17:29]
    (tok_s, tok_r, w_sem, d_sem, wide_sem, tall_sem, zs, zr, gs, gr, o_sem) = refs[29:40]
    width.bind(refs[40:])
    chunks, steps, step = width.chunks, width.steps, width.step
    share, depth = tokens.shape
    rows = t * share
    me = lax.axis_index("tp")
    spots = [lax.rem(me + s, t) for s in range(1, t)]
    sources = [lax.rem(me + t - s, t) for s in range(1, t)]

    def col(v):
        return width.cols(v)

    def load(v, one, two, start):
        slot = lax.rem(v, DEEP)
        for kind, ref in enumerate((one, two)):
            copy = pltpu.make_async_copy(ref.at[:, col(v)], weights.at[slot, kind], w_sem.at[slot, kind])
            if start:
                copy.start()
            else:
                copy.wait()

    def fetch(v):
        @pl.when(v < chunks)
        def _():
            load(v, gate, up, True)

        @pl.when((v >= chunks) & (v < steps))
        def _():
            load(v, along_gate, along_up, True)

    for v in range(DEEP):
        fetch(jnp.int32(v))

    def wide_copies(one, two, c):
        slot = lax.rem(c, SLOTS)
        return [
            pltpu.make_async_copy(ref.at[:, col(c)], wide.at[slot, kind], wide_sem.at[slot, kind])
            for kind, ref in enumerate((one, two))
            if ref is not None
        ]

    def tall_copies(c):
        slot = lax.rem(c, SLOTS)
        return [
            pltpu.make_async_copy(ref.at[col(c), :], tall.at[slot, kind], tall_sem.at[slot, kind])
            for kind, ref in enumerate((along_down, before_down))
        ]

    def open_stream(copies):
        for c in range(min(SLOTS, chunks)):
            for copy in copies(jnp.int32(c)):
                copy.start()

    def turn(copies, c, body):
        for copy in copies(c):
            copy.wait()
        body(c, lax.rem(c, SLOTS))

        @pl.when(c + SLOTS < chunks)
        def _():
            for copy in copies(c + SLOTS):
                copy.start()

    def run_stream(copies, body):
        @pl.loop(0, chunks)
        def _(c):
            turn(copies, c, body)

    gate_stream = functools.partial(wide_copies, along_gate, before_gate)
    up_stream = functools.partial(wide_copies, along_up, before_up)
    again_stream = functools.partial(wide_copies, None, before_gate)
    open_stream(gate_stream)
    load_down = pltpu.make_async_copy(down, downs, d_sem.at[0])
    load_along = pltpu.make_async_copy(along_down, alongs, d_sem.at[1])

    norms[...] = jnp.zeros_like(norms)
    greet(width.partners() + [{"tp": spot} for spot in spots])

    def gather(i):
        return remote(tokens, tok.at[me], tok_s.at[i], tok_r.at[i], {"tp": spots[i]})

    for i in range(t - 1):
        gather(i).start()
    tok[me] = tokens[...]

    def norm_wide(c, slot):
        squares(wide.at[slot, 0], wide.at[slot, 1], norms)

    run_stream(gate_stream, norm_wide)
    open_stream(up_stream)
    for i in range(t - 1):
        gather(i).wait_recv()

    def everyone():
        return tok[...].reshape(rows, depth)

    acc[...] = jnp.zeros_like(acc)

    def front(v):
        load(v, gate, up, False)
        slot = lax.rem(v, DEEP)
        for kind in range(2):
            width.put(v, kind, dot(everyone(), weights[slot, kind]))
        width.mated(v).start()
        fetch(v + DEEP)

    def sums(v):
        one, two = width.totals(v)
        cols = col(v)
        p = width.phase(v)

        @pl.when(p == 0)
        def _():
            keeps[0, :, cols] = one
            keeps[1, :, cols] = two
            width.keep(v, 0, one * jax.nn.sigmoid(one) * two)

        @pl.when(p == 1)
        def _():
            keeps[2, :, cols] = one
            keeps[3, :, cols] = two
            gate_sum, up_sum = keeps[0, :, cols], keeps[1, :, cols]
            logistic = jax.nn.sigmoid(gate_sum)
            slope = logistic * (1.0 + gate_sum * (1.0 - logistic))
            width.keep(v, 1, slope * up_sum * one + gate_sum * logistic * two)

        width.spread(v)

    def middle(v):
        width.complete(v)
        p, at = width.phase(v), col(v)

        @pl.when(v == 0)
        def _():
            load_down.wait()

        @pl.when(v == chunks)
        def _():
            load_along.wait()

        @pl.when(p == 0)
        def _():
            acc[0] += dot(width.rows(v, 0), downs[at, :])

        @pl.when(p == 1)
        def _():
            acc[1] += dot(width.rows(v, 1), downs[at, :]) + dot(width.rows(v, 0), alongs[at, :])

    def z_first(p, i):
        return remote(zx.at[p, spots[i]], zin.at[p, me], zs.at[p, i], zr.at[p, i], {"tp": spots[i]})

    def z_second(p, i):
        return remote(gz.at[p, me], gz.at[p, me], gs.at[p, i], gr.at[p, i], {"tp": spots[i]})

    def z_send(p):
        zx[p] = acc[p].astype(BF16).reshape(t, share, depth)
        for i in range(t - 1):
            z_first(p, i).start()

    def z_finish(p):
        for i in range(t - 1):
            z_first(p, i).wait_recv()
        total = zx[p, me].astype(F32)
        for at in sources:
            total = total + zin[p, at].astype(F32)
        if p == 0:
            total = total - targets[...].astype(F32)
        gz[p, me] = (total / rows).astype(BF16)
        for i in range(t - 1):
            z_second(p, i).start()

    def before_of(kind):
        def body(c, slot):
            bx[kind, :, col(c)] = dot(everyone(), wide[slot, 1]).astype(BF16)

        return body

    def norm_and_before(c, slot):
        norm_wide(c, slot)
        before_of(1)(c, slot)

    def norm_tall(c, slot):
        squares(tall.at[slot, 0], tall.at[slot, 1], norms)

    def unit(v):
        @pl.when(v < chunks)
        def _():
            turn(up_stream, v, norm_and_before)

        @pl.when(v >= chunks)
        def _():
            turn(tall_copies, v - chunks, norm_tall)

    ready = chunks - 1 + LAGS["done"]
    last = steps + LAGS["done"]
    settle = min(ready + 4, last - 1)

    @pl.loop(0, last)
    def _(i):
        staged(i, 0, steps, front)
        staged(i, LAGS["unit"], steps, unit)
        staged(i, LAGS["cross"], steps, width.cross)
        staged(i, LAGS["totals"], steps, sums)
        staged(i, LAGS["relay"], steps, width.relay)
        staged(i, LAGS["last"], steps, width.relay_last)
        staged(i, LAGS["done"], steps, middle)
        staged(i, LAGS["pair"], steps, width.pair)

        @pl.when(i == min(4, ready))
        def _():
            load_down.start()

        @pl.when(i == min(7, ready))
        def _():
            open_stream(tall_copies)

        @pl.when(i == min(11, ready))
        def _():
            load_along.start()

        @pl.when(i == ready)
        def _():
            z_send(0)

        @pl.when(i == settle)
        def _():
            z_finish(0)

    z_send(1)
    open_stream(again_stream)

    stores = [
        pltpu.make_async_copy(tok, out_tokens, o_sem.at[0]),
        pltpu.make_async_copy(width.full, out_units, o_sem.at[1]),
        pltpu.make_async_copy(keeps, out_keeps, o_sem.at[2]),
    ]
    for store in stores:
        store.start()
    run_stream(again_stream, before_of(0))
    stores.append(pltpu.make_async_copy(bx, out_before, o_sem.at[3]))
    stores[-1].start()
    z_finish(1)

    for p in range(2):
        for i in range(t - 1):
            z_second(p, i).wait_recv()
    stores.append(pltpu.make_async_copy(gz, out_grads, o_sem.at[4]))
    stores[-1].start()
    for i in range(t - 1):
        gather(i).wait_send()
        for p in range(2):
            z_first(p, i).wait_send()
            z_second(p, i).wait_send()
    width.drain()
    for store in stores:
        store.wait()


def early(n, t, tokens, targets, gate, up, down, along_gate, along_up, along_down, before_gate, before_up, before_down):
    share, depth = tokens.shape
    width = gate.shape[1]
    rows = t * share
    chunks = width // tile_of(width, max(128, width // 8))
    plan = Width(n, 2, chunks, 2, rows // n, width)
    step = plan.step
    keeps = (4, plan.share, width)
    units = (2, plan.ys, plan.xs, 2, plan.share, width)
    z = (2, t, share, depth)
    return pl.pallas_call(
        functools.partial(early_kernel, n, t, plan),
        out_shape=[
            jax.ShapeDtypeStruct((t, share, depth), BF16),
            jax.ShapeDtypeStruct(units, BF16),
            jax.ShapeDtypeStruct(keeps, F32),
            jax.ShapeDtypeStruct(z, BF16),
            jax.ShapeDtypeStruct((2, rows, width), BF16),
            jax.ShapeDtypeStruct((3, 8, 128), F32),
        ],
        in_specs=[WHOLE, WHOLE] + [ANY] * 9,
        out_specs=[ANY] * 5 + [WHOLE],
        scratch_shapes=[
            VMEM((t, share, depth), BF16),
            VMEM(keeps, F32),
            VMEM((2, rows, width), BF16),
            VMEM((DEEP, 2, depth, step), BF16),
            VMEM((width, depth), BF16),
            VMEM((width, depth), BF16),
            VMEM((SLOTS, 2, depth, step), BF16),
            VMEM((SLOTS, 2, step, depth), BF16),
            VMEM((2, rows, depth), F32),
            VMEM(z, BF16),
            VMEM(z, BF16),
            VMEM(z, BF16),
            DMA((t - 1,)),
            DMA((t - 1,)),
            DMA((DEEP, 2)),
            DMA((2,)),
            DMA((SLOTS, 2)),
            DMA((SLOTS, 2)),
            DMA((2, t - 1)),
            DMA((2, t - 1)),
            DMA((2, t - 1)),
            DMA((2, t - 1)),
            DMA((5,)),
        ]
        + plan.scratch(),
        compiler_params=pltpu.CompilerParams(collective_id=1, has_side_effects=True, vmem_limit_bytes=LIMIT),
    )(tokens, targets, gate, up, down, along_gate, along_up, along_down, before_gate, before_up, before_down)


def late_kernel(n, t, entries, width, *refs):
    (tokens, units, keeps_in, grads_in, before_in, norms, down, along, before) = refs[:9]
    wide_in, beta_prev, out_dirs, scales, alongs, wide_out = refs[9:12], refs[12], refs[13], refs[14], refs[18], refs[19:22]
    tall, hidden, grads = refs[15:18]
    (keeps, bx, downs, befores, sums, gram, swap_gram, mine, box) = refs[22:31]
    (in_sem, m_sem, w_sem, s1, r1) = refs[31:36]
    width.bind(refs[36:])
    chunks, steps, step = width.chunks, width.steps, width.step
    depth = down.shape[1]
    rows = n * width.share
    dp, tp = lax.axis_index("dp"), lax.axis_index("tp")
    everyone, place = n * t, dp * t + tp

    def peer(i):
        at = lax.rem(place + i, everyone)
        return {"dp": lax.div(at, t), "tp": lax.rem(at, t)}

    loads = [
        pltpu.make_async_copy(src, dst, in_sem.at[i])
        for i, (src, dst) in enumerate(((grads_in, grads), (units, hidden), (keeps_in, keeps), (before_in, bx)))
    ]

    def matrix(which, c):
        at, slot = width.cols(c), lax.rem(c, DEEP)
        src = (down, along, before)[which].at[at, :]
        dst = alongs.at[at, :] if which == 1 else (downs, befores)[which // 2].at[slot]
        return pltpu.make_async_copy(src, dst, m_sem.at[which, slot])

    def fetch(c):
        @pl.when(c < steps)
        def _():
            for which in range(3):
                matrix(which, c).start()

    def ahead(c):
        for src, dst, sem in zip(wide_in, wide_out, range(3)):
            at = width.cols(c)
            pltpu.make_async_copy(src.at[:, at], dst.at[:, at], w_sem.at[sem]).start()

    for load in loads:
        load.start()
    for c in range(2):
        fetch(jnp.int32(c))
    sums[...] = jnp.zeros_like(sums)
    gram[...] = jnp.zeros_like(gram)
    swap_gram[...] = jnp.zeros_like(swap_gram)
    tall[...] = tokens[...].reshape(rows, depth).T
    barrier = pltpu.get_barrier_semaphore()

    @pl.loop(1, everyone)
    def _(i):
        pl.semaphore_signal(barrier, inc=1, device_id=peer(i), device_id_type=MESH)

    pl.semaphore_wait(barrier, everyone - 1)
    loads[0].wait()
    for c in range(2, DEEP - 1):
        fetch(jnp.int32(c))
    for load in loads[1:]:
        load.wait()

    def both():
        return grads[...].reshape(2 * rows, depth)

    def unit(v, kind):
        return hidden[kind, :, :, :, :, width.cols(v)].reshape(rows, step)

    def crossed(which, v, products):
        value = products[:rows] * unit(v, 1).astype(F32) + products[rows:] * unit(v, 0).astype(F32)
        sums[which] += lanes(folded(value))

    def back(v):
        matrix(0, v).wait()
        matrix(1, v).wait()
        at = width.cols(v)
        weighted = against(both(), downs[lax.rem(v, DEEP)])
        moved = against(both(), alongs[at, :])
        width.put(v, 0, weighted[:rows])
        width.put(v, 1, weighted[rows:] + moved[:rows])
        width.mated(v).start()
        crossed(1, v, moved)
        fetch(v + DEEP - 1)

    def extra(v):
        matrix(2, v).wait()
        crossed(2, v, against(both(), befores[lax.rem(v, DEEP)]))
        swapped = jnp.concatenate([unit(v, 1), unit(v, 0)])
        swap_gram[...] += against(swapped, swapped)

    def middle(v):
        grad_hidden, grad_hidden_dir = width.totals(v)
        cols = width.cols(v)
        gate_sum, up_sum, gate_dir, up_dir = (keeps[k, :, cols] for k in range(4))
        logistic = jax.nn.sigmoid(gate_sum)
        activation = gate_sum * logistic
        slope = logistic * (1.0 + gate_sum * (1.0 - logistic))
        curve = logistic * (1.0 - logistic) * (2.0 + gate_sum * (1.0 - 2.0 * logistic))
        grad_gate = (
            grad_hidden_dir * up_sum * slope + grad_hidden * up_dir * slope + grad_hidden * up_sum * curve * gate_dir
        ).astype(BF16)
        grad_up = (grad_hidden_dir * activation + grad_hidden * slope * gate_dir).astype(BF16)
        width.keep(v, 0, grad_gate)
        width.keep(v, 1, grad_up)
        width.spread(v)
        sums[1] += lanes(folded(grad_gate.astype(F32) * gate_dir + grad_up.astype(F32) * up_dir))

    def finish(v):
        width.complete(v)
        cols = width.cols(v)
        for kind in range(2):
            part = width.rows(v, kind)
            out_dirs[kind, :, cols] = part
            gram[...] += against(part, part)
            sums[2] += lanes(folded(part.astype(F32) * bx[kind, :, cols].astype(F32)))

    @pl.loop(0, steps + LATER["done"])
    def _(i):
        staged(i, 1, steps, extra)
        staged(i, 0, steps, back)
        staged(i, LATER["cross"], steps, width.cross)
        staged(i, LATER["totals"], steps, middle)
        staged(i, LATER["relay"], steps, width.relay)
        staged(i, LATER["last"], steps, width.relay_last)
        staged(i, LATER["done"], steps, finish)
        staged(i, LATER["pair"], steps, width.pair)
        staged(i, 6, steps, ahead)

    every = tokens[...].reshape(rows, depth)
    sums[0] += lanes(folded(against(every, every) * gram[...])) + lanes(
        folded(against(both(), both()) * swap_gram[...])
    )
    own = [jnp.sum(sums[k]) for k in range(3)] + [jnp.sum(norms[k]) for k in range(3)]
    lane = lax.broadcasted_iota(jnp.int32, (1, 128), 1)
    row = jnp.zeros((1, 128), F32)
    for k in range(6):
        row = jnp.where(lane == k, own[k], row)
    mine[...] = row

    @pl.loop(1, everyone)
    def _(i):
        remote(mine, box.at[place], s1.at[0], r1.at[0], peer(i)).start()

    box[place] = row
    others = box.at[pl.ds(0, everyone - 1)]
    arrivals = remote(others, others, s1.at[0], r1.at[0], peer(1))
    arrivals.wait_recv()
    total = box[...].sum(axis=0)
    image_image, image_along, image_before, along_along, along_before, before_before = (
        jnp.broadcast_to(total[:, k : k + 1], (1, 128)) for k in range(6)
    )
    beta_old = beta_prev[0]
    alpha_coef = image_along / entries
    square = (
        image_image
        - 2.0 * alpha_coef * image_along
        - 2.0 * beta_old * image_before
        + alpha_coef * alpha_coef * along_along
        + 2.0 * alpha_coef * beta_old * along_before
        + beta_old * beta_old * before_before
    )
    beta_coef = jnp.sqrt(square / entries + 1e-06)
    inverse = 1.0 / beta_coef
    scales[0:1] = alpha_coef
    scales[1:2] = beta_coef
    scales[2:3] = inverse
    scales[3:4] = alpha_coef * inverse
    scales[4:5] = beta_old * inverse
    scales[5:8] = jnp.zeros((3, 128), F32)
    arrivals.wait_send()
    width.drain()
    for src, dst, sem in zip(wide_in, wide_out, range(3)):
        pltpu.make_async_copy(src, dst, w_sem.at[sem]).wait()


def late(n, t, entries, tokens, units, keeps, grads, bx, norms, down, along, before, wides, beta_prev):
    width, depth = down.shape
    rows = bx.shape[1]
    chunks = width // tile_of(width, max(128, width // 8))
    plan = Width(n, 1, chunks, 2, rows // n, width)
    small = (8, 128)
    return pl.pallas_call(
        functools.partial(late_kernel, n, t, entries, plan),
        out_shape=[VMEM(bx.shape, BF16), jax.ShapeDtypeStruct(small, F32), VMEM((depth, rows), BF16)]
        + [VMEM(like.shape, BF16) for like in (units, grads, along) + wides],
        in_specs=[WHOLE] + [ANY] * 4 + [WHOLE] + [ANY] * 6 + [pl.BlockSpec(memory_space=pltpu.SMEM)],
        out_specs=[WHOLE] * 9,
        scratch_shapes=[
            VMEM(keeps.shape, F32),
            VMEM(bx.shape, BF16),
            VMEM((DEEP, plan.step, depth), BF16),
            VMEM((DEEP, plan.step, depth), BF16),
            VMEM((3,) + small, F32),
            VMEM((rows, rows), F32),
            VMEM((2 * rows, 2 * rows), F32),
            VMEM((1, 128), F32),
            VMEM((n * t, 1, 128), F32),
            DMA((4,)),
            DMA((3, DEEP)),
            DMA((3,)),
            DMA((1,)),
            DMA((1,)),
        ]
        + plan.scratch(),
        compiler_params=pltpu.CompilerParams(collective_id=2, has_side_effects=True, vmem_limit_bytes=LATE),
    )(tokens, units, keeps, grads, bx, norms, down, along, before, *wides, beta_prev)


def next_kernel(scales, before_up, before_down, dirs, tall, units, grads, along_down, along_gate, along_up, before_gate, *refs):
    out_gate, out_up, out_down, coefs, slopes, ups, downs, wides, talls, b_sem, o_sem = refs
    inverse, alpha, beta = scales[2, 0], scales[3, 0], scales[4, 0]
    depth, width = along_gate.shape
    rows = dirs.shape[1]
    tile, part, deep = wides.shape[2], tile_of(depth, 256), downs.shape[0]
    count = width // tile

    def piece(j):
        return pl.ds(pl.multiple_of(j * tile, tile), tile)

    def previous(which, j):
        if which == 0:
            return pltpu.make_async_copy(before_up.at[:, piece(j)], ups.at[:, piece(j)], b_sem.at[0, j])
        slot = lax.rem(j, deep)
        return pltpu.make_async_copy(before_down.at[piece(j), :], downs.at[slot], b_sem.at[1, slot])

    for j in range(count):
        previous(0, jnp.int32(j)).start()
    coefs[0] = scales[0, 0]
    coefs[1] = scales[1, 0]

    def scaled(values):
        return (values.astype(F32) * inverse).astype(BF16)

    def blend(image, along, before):
        return (image - along.astype(F32) * alpha - before.astype(F32) * beta).astype(BF16)

    def store(which, j):
        slot = lax.rem(j, DEEP)
        if which < 2:
            dst, src = (out_gate, out_up)[which].at[:, piece(j)], wides.at[slot]
        else:
            dst, src = out_down.at[piece(j), :], talls.at[slot]
        return pltpu.make_async_copy(src, dst, o_sem.at[which // 2, slot])

    for which, (along, before) in enumerate(((along_gate, before_gate), (along_up, ups))):
        @pl.loop(0, count)
        def _(j):
            slot, cols = lax.rem(j, DEEP), piece(j)
            if which == 0:
                @pl.when(j >= DEEP)
                def _():
                    store(0, j).wait()

                @pl.when(j == count // 2)
                def _():
                    for at in range(min(deep, count)):
                        previous(1, jnp.int32(at)).start()
            else:
                previous(0, j).wait()
                store(0, j).wait()
            way = scaled(dirs[which, :, cols])
            for at in range(0, depth, part):
                here = slice(at, at + part)
                wides[slot, here, :] = blend(dot(tall[here, :], way), along[here, cols], before[here, cols])
            store(which, j).start()

    slopes[...] = scaled(grads[...].reshape(2 * rows, depth))

    @pl.loop(0, count)
    def _(j):
        slot, cols = lax.rem(j, DEEP), piece(j)
        place = lax.rem(j, deep)

        @pl.when(j >= DEEP)
        def _():
            store(2, j).wait()

        previous(1, j).wait()
        swapped = jnp.concatenate([units[k, :, :, :, :, cols].reshape(rows, tile) for k in (1, 0)]).T
        for at in range(0, depth, part):
            here = slice(at, at + part)
            talls[slot, :, here] = blend(dot(swapped, slopes[:, here]), along_down[cols, here], downs[place, :, here])
        store(2, j).start()

        @pl.when(j + deep < count)
        def _():
            previous(1, j + deep).start()

    for j in range(min(DEEP, count)):
        store(0, jnp.int32(j)).wait()
        store(2, jnp.int32(j)).wait()


def next_parts(scales, before_up, before_down, *held):
    depth, width = before_up.shape
    rows = held[0].shape[1]
    tile = tile_of(width, max(128, min(256, width // DEEP)))
    smem = pl.BlockSpec(memory_space=pltpu.SMEM)
    count = width // tile
    deep = min(2 * DEEP, count)
    return pl.pallas_call(
        next_kernel,
        out_shape=[jax.ShapeDtypeStruct((depth, width), BF16)] * 2
        + [jax.ShapeDtypeStruct((width, depth), BF16), jax.ShapeDtypeStruct((2,), F32)],
        in_specs=[smem] + [ANY] * 2 + [WHOLE] * len(held),
        out_specs=[ANY] * 3 + [smem],
        scratch_shapes=[
            VMEM((2 * rows, depth), BF16),
            VMEM((depth, width), BF16),
            VMEM((deep, tile, depth), BF16),
            VMEM((DEEP, depth, tile), BF16),
            VMEM((DEEP, tile, depth), BF16),
            DMA((2, count)),
            DMA((2, DEEP)),
        ],
        compiler_params=pltpu.CompilerParams(vmem_limit_bytes=LAST),
    )(scales, before_up, before_down, *held)


def on_device(
    n,
    t,
    tokens,
    targets,
    gate_weight,
    up_weight,
    down_weight,
    direction_gate,
    direction_up,
    direction_down,
    previous_gate,
    previous_up,
    previous_down,
    beta_prev,
):
    everyone, units, keeps, grads, bx, norms = early(
        n,
        t,
        tokens,
        targets,
        gate_weight,
        up_weight,
        down_weight,
        direction_gate,
        direction_up,
        direction_down,
        previous_gate,
        previous_up,
        previous_down,
    )
    entries = float(n * t * (gate_weight.size + up_weight.size + down_weight.size))
    wides = (direction_gate, direction_up, previous_gate)
    dirs, scales, *held = late(
        n, t, entries, everyone, units, keeps, grads, bx, norms, down_weight, direction_down, previous_down, wides, beta_prev
    )
    held = [pltpu.with_memory_space_constraint(array, VMEM) for array in [dirs] + held]
    return tuple(next_parts(scales, previous_up, previous_down, *held))


def solution(mesh):
    wide, tall = P("dp", "tp"), P("tp", "dp")
    in_specs = (tall, tall, wide, wide, tall, wide, wide, tall, wide, wide, tall, P())
    return jax.shard_map(
        functools.partial(on_device, mesh.shape["dp"], mesh.shape["tp"]),
        mesh=mesh,
        in_specs=in_specs,
        out_specs=(wide, wide, tall, P()),
        check_vma=False,
    )
```
